32 devices in a mesh: chan: 4 (over x, core), bl: 8 (over z, y).
Axes of the slice: x: 2, y: 2, z: 4, core: 2. Of those that a mesh axis runs over, the one named last changes fastest.
Arguments:
- vis_value: bfloat16 [4, 8, 2, 2048], P('chan', 'bl'), may hold values from -6 to 6
- vis_weight: bfloat16 [4, 8, 2048], P('chan', 'bl'), may hold values from 0.19921875 to 5
- kernel: bfloat16 [4, 8, 64, 2048], P('chan', 'bl'), may hold values from 0.049804688 to 1
- tile_index: int32 [4, 8, 2048], P('chan', 'bl'), may hold values from 0 to 262143
- plane_index: int32 [4, 8, 2048], P('chan', 'bl'), may hold values from 0 to 7
- chan_index: int32 [4, 8, 2048], P('chan', 'bl'), may hold values from 0 to 15
- chan_offset: float32 [4, 16], P('chan'), may hold values from -0.4 to 0.4
- counts: int32 [4, 8], P('chan', 'bl'), may hold values from 256 to 2048, as said below
Outputs:
- taylor_coeffs: float32 [3, 32768], P(None, ('chan', 'bl'))
The draws below stay inside these ranges and needn't reach their ends.
Inputs may be any that keep to these rules, and one draw needn't show every extreme that they name: `counts`: each device's number of live visibility slots; slots from that number on are ignored. In every draw some device has exactly 2048.
All inputs are finite; a program needn't handle non-finite values.
Results may differ from the reference program's by a relative error of at most 0.0003.
Values may be sent and summed in bfloat16 or wider, within the bound.
A program may use at most 128 MiB of HBM per device.

```python
import math
import jax
import jax.numpy as jnp
from jax import lax

NPIX = 4096
TILE = 8
NTILE = 512
TAYLOR = 3
MOMENTS = 5
WPLANES = 8
CH_DEV = 16
STRIP = 8
SLOTS = 2048
BLK = 256
N_CHAN = 4
N_BL = 8


def draw_counts(key, part):
    raw = jax.random.randint(jax.random.fold_in(key, 11), (N_CHAN, N_BL), 0, 1000)
    spread = raw * raw // 1000 * (SLOTS - BLK) // 1000
    base_counts = (BLK + spread).reshape(-1)
    chosen = jax.random.randint(jax.random.fold_in(key, 12), (), 0, N_CHAN * N_BL)
    filled = jnp.where(jnp.arange(N_CHAN * N_BL) == chosen, SLOTS, base_counts)
    return filled.reshape(N_CHAN, N_BL).astype(jnp.int32)


def place_ends(values, key, least, high):
    dims = values.shape
    index_at = [jax.random.randint(jax.random.fold_in(key, axis), (), 0, dims[axis]) for axis in range(len(dims))]
    values = values.at[tuple(index_at)].set(least)
    longest = dims.index(max(dims))
    index_at[longest] = (index_at[longest] + 1) % dims[longest]
    return values.at[tuple(index_at)].set(high)


def block_levels(stream_key, dims, pieces, least, top_value):
    def one(axis_at, shards_of):
        draws = jax.random.uniform(jax.random.fold_in(jax.random.fold_in(stream_key, 6), axis_at), (shards_of,), jnp.float32, least / len(pieces), top_value / len(pieces))
        return jnp.repeat(jnp.exp(draws), dims[axis_at] // shards_of).reshape((-1,) + (1,) * (len(dims) - axis_at - 1))

    gain = one(*pieces[0])
    for cut in pieces[1:]:
        gain = gain * one(*cut)
    return gain


def scatter_about(stream_key, shape, width, limit, cuts=(), kind=jnp.bfloat16):
    result = jax.random.normal(stream_key, shape, jnp.float32) * width
    if len(cuts) > 0:
        result = block_levels(stream_key, shape, cuts, -0.22, 0.18) * result
    return jnp.clip(result, min=-limit, max=limit).astype(kind)


def setup_inputs(seed: int = 0) -> dict:
    arg_keys = jax.random.split(jax.random.key(seed), 9)
    vis_value = scatter_about(arg_keys[0], (N_CHAN, N_BL, 2, SLOTS), 1.0, 6.0, ((0, 4), (1, 8)))
    vis_weight = jnp.clip(jnp.exp(math.log(5.0) - 3.2227897 * jax.random.uniform(arg_keys[1], (N_CHAN, N_BL, SLOTS), jnp.float32) ** block_levels(arg_keys[1], (N_CHAN, N_BL, SLOTS), ((0, 4), (1, 8)), -0.2, 0.2)), 0.19921875, 5.0).astype(jnp.bfloat16)
    kernel = jnp.clip(0.049804688 + 0.9501953 * jax.random.uniform(arg_keys[2], (N_CHAN, N_BL, TILE * TILE, SLOTS), jnp.float32) ** block_levels(arg_keys[2], (N_CHAN, N_BL, TILE * TILE, SLOTS), ((0, 4), (1, 8)), -0.2, 0.2), 0.049804688, 1.0).astype(jnp.bfloat16)
    tile_index = place_ends(jax.random.randint(arg_keys[3], (N_CHAN, N_BL, SLOTS), 0, NTILE * NTILE), jax.random.fold_in(arg_keys[3], 1), 0, (NTILE * NTILE) - 1).astype(jnp.int32)
    plane_index = place_ends(jax.random.randint(arg_keys[4], (N_CHAN, N_BL, SLOTS), 0, WPLANES), jax.random.fold_in(arg_keys[4], 1), 0, WPLANES - 1).astype(jnp.int32)
    chan_index = place_ends(jax.random.randint(arg_keys[5], (N_CHAN, N_BL, SLOTS), 0, CH_DEV), jax.random.fold_in(arg_keys[5], 1), 0, CH_DEV - 1).astype(jnp.int32)
    chan_offset = jnp.clip(jax.random.uniform(arg_keys[6], (N_CHAN, CH_DEV), jnp.float32, -0.4, 0.4) * block_levels(arg_keys[6], (N_CHAN, CH_DEV), ((0, 4),), -0.4, 0.0), -0.4, 0.4)
    counts = draw_counts(jax.random.fold_in(arg_keys[8], 71), 0)
    return dict(vis_value=vis_value, vis_weight=vis_weight, kernel=kernel, tile_index=tile_index, plane_index=plane_index, chan_index=chan_index, chan_offset=chan_offset, counts=counts)


two_pi = 6.283185307179586
w_step = 40.0

def device_terms(values, weights, kernel, tiles, planes, chans, offsets, live_count):
    slot_count = weights.shape[0]
    ntiles = NPIX // TILE
    live_mask = jnp.arange(slot_count, dtype=jnp.int32) < live_count
    channel_ids = jnp.arange(CH_DEV, dtype=jnp.int32)
    taylor_coord = lax.optimization_barrier(jnp.sum(jnp.where(chans[:, None] == channel_ids[None, :], offsets[None, :], 0.0), axis=1))
    live_weight = jnp.where(live_mask, weights.astype(jnp.float32), 0.0)
    kernel_taps = kernel.astype(jnp.float32).reshape(TILE, TILE, slot_count)
    strip_rows = jnp.arange(STRIP, dtype=jnp.int32) - STRIP // 2
    grid_cols = (tiles // ntiles)[:, None] * TILE + jnp.arange(TILE, dtype=jnp.int32)[None, :] - NPIX // 2
    phase_index = grid_cols[:, :, None] * strip_rows[None, None, :] % NPIX
    phase_angle = phase_index.astype(jnp.float32) * (two_pi / NPIX)
    tile_real = jnp.einsum('abj,jal->jlb', kernel_taps, jnp.cos(phase_angle), precision=lax.Precision.HIGHEST)
    tile_imag = jnp.einsum('abj,jal->jlb', kernel_taps, jnp.sin(phase_angle), precision=lax.Precision.HIGHEST)
    base_real = live_weight * values[0].astype(jnp.float32)
    base_imag = live_weight * values[1].astype(jnp.float32)
    power_list = [jnp.ones_like(taylor_coord)]
    for power_id in range(MOMENTS - 1):
        power_list.append(power_list[power_id] * taylor_coord)
    power_stack = jnp.stack(power_list[:TAYLOR], axis=1)
    coeff_real = base_real[:, None] * power_stack
    coeff_imag = base_imag[:, None] * power_stack
    part_real = coeff_real[:, :, None, None] * tile_real[:, None] - coeff_imag[:, :, None, None] * tile_imag[:, None]
    part_imag = coeff_real[:, :, None, None] * tile_imag[:, None] + coeff_imag[:, :, None, None] * tile_real[:, None]
    updates = jnp.stack([part_real, part_imag], axis=-1).reshape(slot_count, TAYLOR * STRIP * TILE * 2)
    target_rows = planes * ntiles + tiles % ntiles
    tap_sums = lax.optimization_barrier(jnp.sum(kernel_taps, axis=(0, 1)))
    weighted_taps = live_weight * tap_sums
    moment_add = jnp.stack([jnp.sum(weighted_taps * power_list[moment_id]) for moment_id in range(MOMENTS)])
    return (updates, target_rows, moment_add)

def screen_angle(plane_ids, column_ids):
    cell_size = 0.5 / NPIX
    strip_rows = jnp.arange(STRIP, dtype=jnp.int32) - STRIP // 2
    xcoord = strip_rows.astype(jnp.float32) * cell_size
    ycoord = (column_ids - NPIX // 2).astype(jnp.float32) * cell_size
    radius = xcoord[:, None] * xcoord[:, None] + ycoord[None, :] * ycoord[None, :]
    lowered = -radius / (1.0 + jnp.sqrt(1.0 - radius))
    w_value = w_step * (plane_ids.astype(jnp.float32) - 0.5 * (WPLANES - 1))
    return two_pi * w_value[:, None, None] * lowered[None]

def solve_taylor(moments, images):
    entry_00, entry_01, entry_02 = (moments[0], moments[1], moments[2])
    entry_11, entry_12, entry_22 = (moments[2], moments[3], moments[4])
    minor_00 = entry_11 * entry_22 - entry_12 * entry_12
    minor_01 = entry_02 * entry_12 - entry_01 * entry_22
    minor_02 = entry_01 * entry_12 - entry_02 * entry_11
    minor_11 = entry_00 * entry_22 - entry_02 * entry_02
    minor_12 = entry_01 * entry_02 - entry_00 * entry_12
    minor_22 = entry_00 * entry_11 - entry_01 * entry_01
    determinant = entry_00 * minor_00 + entry_01 * minor_01 + entry_02 * minor_02
    first = (minor_00 * images[0] + minor_01 * images[1] + minor_02 * images[2]) / determinant
    second = (minor_01 * images[0] + minor_11 * images[1] + minor_12 * images[2]) / determinant
    third = (minor_02 * images[0] + minor_12 * images[1] + minor_22 * images[2]) / determinant
    return jnp.stack([first, second, third])

def reference(vis_value, vis_weight, kernel, tile_index, plane_index, chan_index, chan_offset, counts):
    device_total = N_CHAN * N_BL
    slot_count = vis_weight.shape[-1]
    ntiles = NPIX // TILE
    offsets_all = jnp.repeat(chan_offset, N_BL, axis=0)
    inputs = (vis_value.reshape(device_total, 2, slot_count), vis_weight.reshape(device_total, slot_count), kernel.reshape(device_total, TILE * TILE, slot_count), tile_index.reshape(device_total, slot_count), plane_index.reshape(device_total, slot_count), chan_index.reshape(device_total, slot_count), offsets_all, counts.reshape(device_total))

    def accumulate(state_pair, sliced):
        uv_grid, moments = state_pair
        updates, target_rows, moment_add = device_terms(*sliced)
        return ((uv_grid.at[target_rows].add(updates), moments + moment_add), None)
    initial = (jnp.zeros((WPLANES * ntiles, TAYLOR * STRIP * TILE * 2), jnp.float32), jnp.zeros((MOMENTS,), jnp.float32))
    (uv_grid, moments), unused = lax.scan(accumulate, initial, inputs)
    cube = uv_grid.reshape(WPLANES, ntiles, TAYLOR, STRIP, TILE, 2)
    cube = jnp.transpose(cube, (0, 2, 3, 1, 4, 5)).reshape(WPLANES, TAYLOR, STRIP, NPIX, 2)
    column_ids = jnp.arange(NPIX, dtype=jnp.int32)
    parity = 1.0 - 2.0 * (column_ids % 2).astype(jnp.float32)
    spectrum = (cube[..., 0] + 1j * cube[..., 1]) * parity
    transformed = jnp.fft.ifft(spectrum, axis=-1) * NPIX
    angles = screen_angle(jnp.arange(WPLANES, dtype=jnp.int32), column_ids)
    image = lax.optimization_barrier(jnp.sum(parity * (jnp.real(transformed) * jnp.cos(angles)[:, None] - jnp.imag(transformed) * jnp.sin(angles)[:, None]), axis=0))
    return solve_taylor(moments, image.reshape(TAYLOR, STRIP * NPIX))
```

```python
import functools

import numpy as np
import jax
import jax.numpy as jnp
from jax import lax
from jax.experimental import pallas as pl
from jax.experimental.pallas import tpu as pltpu
from jax.sharding import PartitionSpec as P

NPIX = 4096
TILE = 8
TAYLOR = 3
MOMENTS = 5
WPLANES = 8
STRIP = 8
LANES = 128
CORES = 2

two_pi = 2.0 * np.pi
w_step = 40.0
ntiles = NPIX // TILE
planes = WPLANES // 2
held = STRIP // CORES
quads = ntiles // LANES
groups = planes * quads // 2
pairs = TILE // 2
per_k = TILE * STRIP + 8
rows_all = TAYLOR * per_k
BLK = 512
MESH = pl.DeviceIdType.MESH


def split(x):
    high = x.astype(jnp.bfloat16)
    low = (x - high.astype(jnp.float32)).astype(jnp.bfloat16)
    return high, low


def cosine_series():
    g = 0.125 - 0.125 * np.cos(np.pi * (np.arange(64) + 0.5) / 64)
    fit = np.polynomial.Polynomial.fit(g, np.cos(two_pi * np.sqrt(g)), 8, domain=[0.0, 0.25])
    return [float(c) for c in fit.convert().coef]


cos_terms = cosine_series()


@functools.cache
def tables(n_chan):
    f32 = np.float32
    bf16 = jnp.bfloat16
    per = STRIP // n_chan

    def two(x):
        x = x.astype(f32)
        high = x.astype(bf16)
        return high, (x - high.astype(f32)).astype(bf16)

    slot = np.arange(held)
    strips = [(slot // per * CORES + core) * per + slot % per for core in range(CORES)]
    sub_e = np.arange(8) // held
    sub_l = np.arange(8) % held

    taps = np.zeros((CORES, 88, 2, TILE, TILE))
    for core in range(CORES):
        offset = strips[core] - STRIP // 2
        angle = two_pi * np.arange(TILE)[None, :] * offset[:, None] / NPIX
        for e in range(TILE + 1):
            for part, wave in enumerate((np.cos(angle), np.sin(angle))):
                if e < TILE:
                    rows = [part * 32 + e // 2 * 8 + e % 2 * held + slot]
                else:
                    rows = [64 + part * 8 + slot, 64 + part * 8 + held + slot]
                for row in rows:
                    if e < TILE:
                        taps[core, row, 0, :, e] = wave
                    if e > 0:
                        taps[core, row, 1, :, TILE - e] = wave
    taps[:, 80:] = 1.0
    tap_high, tap_low = two(taps.reshape(CORES, 88, 2 * TILE * TILE))
    tap_table = np.concatenate([tap_high, tap_low], axis=2)

    ids = np.arange(LANES)
    angle = two_pi * (ids[:, None] * ids[None, :] % LANES) / LANES
    cosine, sine = np.cos(angle), np.sin(angle)
    coarse = np.stack(two(np.block([[cosine, sine], [-sine, cosine]])))

    cell = (8 * np.arange(quads)[:, None, None] + 2 * np.arange(pairs)[None, :, None] + sub_e[None, None, :])[..., None]
    angle = two_pi * cell * ids / NPIX
    sign = 1.0 - 2.0 * ((cell + ids) % 2)
    twist = np.stack([np.cos(angle) * sign, np.sin(angle) * sign], axis=2)
    e = 2 * np.arange(pairs)[None, :, None] + sub_e[None, None, :]
    angle = np.broadcast_to(two_pi * (np.arange(4)[:, None, None] * e)[..., None] / 32, (4, pairs, 8, LANES))
    inner = np.stack([np.cos(angle), np.sin(angle)], axis=2)
    twist = np.stack([twist, inner]).astype(f32)

    cell_size = 0.5 / NPIX
    screens = []
    for core in range(CORES):
        x = (strips[core][sub_l] - STRIP // 2) * cell_size
        column = ids[None, None, :] + LANES * (np.arange(16)[:, None, None] + 16 * sub_e[None, :, None])
        y = (column - NPIX // 2) * cell_size
        radius = x[None, :, None] ** 2 + y**2
        lowered = -radius / (1.0 + np.sqrt(1.0 - radius))
        w = w_step * (np.arange(planes) - 0.5 * (WPLANES - 1))
        angle = two_pi * w[:, None, None, None] * lowered[None]
        screens.append(np.stack([np.cos(angle), np.sin(angle)], axis=2))
    screen = np.stack(screens).astype(f32)
    return tap_table, coarse, twist, screen


def solve_taylor(moments, images):
    entry_00, entry_01, entry_02 = (moments[0], moments[1], moments[2])
    entry_11, entry_12, entry_22 = (moments[2], moments[3], moments[4])
    minor_00 = entry_11 * entry_22 - entry_12 * entry_12
    minor_01 = entry_02 * entry_12 - entry_01 * entry_22
    minor_02 = entry_01 * entry_12 - entry_02 * entry_11
    minor_11 = entry_00 * entry_22 - entry_02 * entry_02
    minor_12 = entry_01 * entry_02 - entry_00 * entry_12
    minor_22 = entry_00 * entry_11 - entry_01 * entry_01
    determinant = entry_00 * minor_00 + entry_01 * minor_01 + entry_02 * minor_02
    first = (minor_00 * images[0] + minor_01 * images[1] + minor_02 * images[2]) / determinant
    second = (minor_01 * images[0] + minor_11 * images[1] + minor_12 * images[2]) / determinant
    third = (minor_02 * images[0] + minor_12 * images[1] + minor_22 * images[2]) / determinant
    return first, second, third


def multiply(a, b):
    return a[0] * b[0] - a[1] * b[1], a[0] * b[1] + a[1] * b[0]


def radix4(x):
    a = (x[0][0] + x[2][0], x[0][1] + x[2][1])
    b = (x[0][0] - x[2][0], x[0][1] - x[2][1])
    c = (x[1][0] + x[3][0], x[1][1] + x[3][1])
    d = (x[1][0] - x[3][0], x[1][1] - x[3][1])
    return (
        (a[0] + c[0], a[1] + c[1]), (b[0] - d[1], b[1] + d[0]),
        (a[0] - c[0], a[1] - c[1]), (b[0] + d[1], b[1] - d[0]),
    )


def strip_kernel(
    n_chan, n_bl, count_ref, offset_ref, value_ref, weight_ref, kernel_ref, tile_ref, plane_ref, chan_ref,
    tap_hbm, coarse_hbm, twist_hbm, screen_hbm, out_ref,
    tap_ref, coarse_ref, twist_ref, screen_ref, meta_ref, meta_land, taps_land,
    high_ref, low_ref, dist_ref, grid_ref, mom_ref, spec_ref, acc_ref, img0_ref, img1_ref, img2_ref,
    xland_ref, sum_ref, bland_ref, msend_ref, mxland_ref, msum_ref, mbland_ref,
    load_sem, pair_send, pair_recv, x_send, x_recv, xm_send, xm_recv, b_send, b_recv, bm_send, bm_recv,
):
    chan = lax.axis_index("chan")
    bl = lax.axis_index("bl")
    core = lax.rem(chan, CORES)
    seat = chan // CORES
    n_seat = n_chan // CORES
    per = STRIP // n_chan
    img_refs = (img0_ref, img1_ref, img2_ref)
    slots = kernel_ref.shape[1]

    def seat_peer(d):
        return lax.rem(seat + d, n_seat)

    def bl_peer(d):
        return lax.rem(bl + d, n_bl)

    mate = (chan + 1 - 2 * core, bl)
    barrier = pltpu.get_barrier_semaphore()
    pl.semaphore_signal(barrier, inc=1, device_id=mate, device_id_type=MESH)
    for d in range(1, n_seat):
        pl.semaphore_signal(barrier, inc=1, device_id=(seat_peer(d) * CORES + core, bl), device_id_type=MESH)
    for d in range(1, n_bl):
        pl.semaphore_signal(barrier, inc=1, device_id=(chan, bl_peer(d)), device_id_type=MESH)

    loads = [
        pltpu.make_async_copy(source, target, load_sem.at[i])
        for i, (source, target) in enumerate((
            (tap_hbm.at[core], tap_ref), (coarse_hbm, coarse_ref),
            (twist_hbm, twist_ref), (screen_hbm.at[core], screen_ref),
        ))
    ]
    for load in loads:
        load.start()

    grid_ref[...] = jnp.zeros_like(grid_ref)
    mom_ref[...] = jnp.zeros_like(mom_ref)

    slot = lax.broadcasted_iota(jnp.int32, (1, slots), 1)
    tiles = tile_ref[...]
    plane = plane_ref[...]
    chans = chan_ref[...]
    coord = jnp.zeros((1, slots), jnp.float32)
    for c in range(offset_ref.shape[1]):
        coord = jnp.where(chans == c, offset_ref[0, c], coord)
    weight = jnp.where(slot < count_ref[0, 0], weight_ref[...].astype(jnp.float32), 0.0)
    value = value_ref[...].astype(jnp.float32)
    flip = plane >= planes
    v_tile = tiles & (ntiles - 1)
    v_tile = jnp.where(flip, ntiles - 1 - v_tile, v_tile)
    fold = jnp.where(flip, WPLANES - 1 - plane, plane)
    place = (fold * quads + (v_tile & (quads - 1))) * LANES + lax.shift_right_logical(v_tile, quads.bit_length() - 1)
    meta_ref[0:1, :] = weight * value[0:1]
    meta_ref[1:2, :] = weight * value[1:2]
    meta_ref[2:3, :] = coord
    meta_ref[3:4, :] = weight
    meta_ref[4:5, :] = (lax.shift_right_logical(tiles, ntiles.bit_length() - 1) - ntiles // 2).astype(jnp.float32)
    meta_ref[5:6, :] = place.astype(jnp.float32)
    meta_ref[6:7, :] = jnp.where(flip, -1.0, 1.0)
    meta_ref[7:8, :] = jnp.zeros((1, slots), jnp.float32)

    sub = lax.broadcasted_iota(jnp.int32, (8, 1), 0)
    first = sub < held
    local = lax.rem(sub, held)
    strip = (local // per * CORES + core) * per + lax.rem(local, per) - STRIP // 2
    turn = strip.astype(jnp.float32) * (1.0 / ntiles)
    quarter = jnp.where(first, 0.0, 0.25)

    loads[0].wait()

    def one_block(taps_ref, rows_ref, block, carry):
        here = pl.ds(pl.multiple_of(block * BLK, BLK), BLK)
        base_real = rows_ref[0:1, here]
        base_imag = rows_ref[1:2, here]
        coord = rows_ref[2:3, here]
        weight = rows_ref[3:4, here]
        u_off = rows_ref[4:5, here]
        place = rows_ref[5:6, here]
        sign = rows_ref[6:7, here]
        taps = taps_ref[:, here]
        plain = taps * jnp.maximum(sign, 0.0).astype(jnp.bfloat16)
        turned = taps * jnp.maximum(-sign, 0.0).astype(jnp.bfloat16)
        sums = jnp.dot(
            tap_ref[...], jnp.concatenate([plain, turned, plain, turned], axis=0),
            preferred_element_type=jnp.float32,
        )
        cycle = u_off * turn - quarter
        cycle = cycle - jnp.floor(cycle + 0.5)
        square = cycle * cycle
        wave = jnp.full_like(square, cos_terms[-1])
        for term in cos_terms[-2::-1]:
            wave = wave * square + term
        other = pltpu.roll(wave, held, 0)
        cosine = jnp.where(first, wave, other)
        sine = jnp.where(first, other, wave)
        z_real = base_real * cosine - base_imag * sine
        z_imag = base_real * sine + base_imag * cosine
        s_real = z_real * sign
        s_imag = z_imag * sign
        sum_real = sums[0:32].reshape(pairs, 8, BLK)
        sum_imag = sums[32:64].reshape(pairs, 8, BLK)
        part_real = (sum_real * z_real[None] - sum_imag * z_imag[None]).reshape(32, BLK)
        part_imag = (sum_real * s_imag[None] + sum_imag * s_real[None]).reshape(32, BLK)
        edge = sums[64:72] * jnp.where(first, z_real, s_imag) + sums[72:80] * jnp.where(first, -z_imag, s_real)
        part = jnp.concatenate([part_real, part_imag, edge], axis=0)
        parts = [part]
        for k in range(1, TAYLOR):
            parts.append(parts[-1] * coord)
        high, low = split(jnp.concatenate(parts, axis=0))
        high_ref[...] = high
        low_ref[...] = low

        weighted = weight * sums[80:81]
        power = weighted
        for m in range(MOMENTS):
            mom_ref[m : m + 1, :] += power
            power = power * coord

        lane = lax.broadcasted_iota(jnp.int32, (BLK, LANES), 1).astype(jnp.float32)
        column = jnp.transpose(jnp.broadcast_to(place, (LANES, BLK)))
        dist_ref[...] = column - lane
        for g in range(groups):
            hot = jnp.concatenate(
                [jnp.where(dist_ref[...] == float((2 * g + h) * LANES), 1.0, 0.0) for h in range(2)], axis=1
            ).astype(jnp.bfloat16)
            grid_ref[g] += jnp.dot(high_ref[...], hot, preferred_element_type=jnp.float32) + jnp.dot(
                low_ref[...], hot, preferred_element_type=jnp.float32
            )
        return carry

    blocks = slots // BLK
    lax.fori_loop(0, blocks // 2, functools.partial(one_block, kernel_ref, meta_ref), 0)
    pl.semaphore_wait(barrier, 1 + n_seat - 1 + n_bl - 1)
    swaps = [
        pltpu.make_async_remote_copy(
            src_ref=source, dst_ref=target, send_sem=pair_send.at[i], recv_sem=pair_recv.at[i],
            device_id=mate, device_id_type=MESH,
        )
        for i, (source, target) in enumerate(((kernel_ref, taps_land), (meta_ref, meta_land)))
    ]
    for swap in swaps:
        swap.start()
    lax.fori_loop(blocks // 2, blocks, functools.partial(one_block, kernel_ref, meta_ref), 0)
    for swap in swaps:
        swap.wait()
    lax.fori_loop(0, blocks, functools.partial(one_block, taps_land, meta_land), 0)

    msend_ref[...] = jnp.broadcast_to(jnp.sum(mom_ref[...], axis=1, keepdims=True), msend_ref.shape)
    mom_x = [
        pltpu.make_async_remote_copy(
            src_ref=msend_ref, dst_ref=mxland_ref.at[d], send_sem=xm_send.at[d], recv_sem=xm_recv.at[d],
            device_id=(seat_peer(d) * CORES + core, bl), device_id_type=MESH,
        )
        for d in range(1, n_seat)
    ]
    for copy in mom_x:
        copy.start()

    for load in loads[1:]:
        load.wait()
    flipper = jnp.where(first, 1.0, -1.0)
    spin = [
        (jnp.where(first, 1.0, float(np.cos(two_pi * s / 8))), jnp.where(first, 0.0, float(np.sin(two_pi * s / 8))))
        for s in range(4)
    ]

    def transform(k):
        low_row = k * per_k
        pieces = []
        for p in range(planes):
            edges = []
            for b in range(quads):
                q = p * quads + b
                lanes = pl.ds(q % 2 * LANES, LANES)
                edges.append(grid_ref[q // 2, low_row + 64 : low_row + 72, lanes])
            edges = [pltpu.roll(edges[-1], 1, 1)] + edges[:-1]
            for b in range(quads):
                q = p * quads + b
                lanes = pl.ds(q % 2 * LANES, LANES)
                real = grid_ref[q // 2, low_row : low_row + 32, lanes]
                imag = grid_ref[q // 2, low_row + 32 : low_row + 64, lanes]
                edge = edges[b]
                head_real = real[:8] + jnp.where(first, edge, 0.0)
                head_imag = imag[:8] + jnp.where(first, pltpu.roll(edge, held, 0), 0.0)
                real = jnp.concatenate([head_real, real[8:]], axis=0)
                imag = jnp.concatenate([head_imag, imag[8:]], axis=0)
                pieces.append(jnp.concatenate([real, imag], axis=1))
        high, low = split(jnp.concatenate(pieces, axis=0))
        spec_ref[...] = (
            jnp.dot(high, coarse_ref[0], preferred_element_type=jnp.float32)
            + jnp.dot(high, coarse_ref[1], preferred_element_type=jnp.float32)
            + jnp.dot(low, coarse_ref[0], preferred_element_type=jnp.float32)
        )
        acc_ref[...] = jnp.zeros_like(acc_ref)

        def one_plane(p, carry):
            inner = [[None] * pairs for r in range(4)]
            for t in range(pairs):
                column = []
                for b in range(quads):
                    row = pl.ds(pl.multiple_of((p * quads + b) * 32 + t * 8, 8), 8)
                    x = (spec_ref[row, :LANES], spec_ref[row, LANES:])
                    column.append(multiply(x, (twist_ref[0, b, t, 0], twist_ref[0, b, t, 1])))
                for r, z in enumerate(radix4(column)):
                    inner[r][t] = multiply(z, (twist_ref[1, r, t, 0], twist_ref[1, r, t, 1])) if r else z
            for r in range(4):
                for s, z in enumerate(radix4(inner[r])):
                    if s:
                        z = multiply(z, spin[s])
                    real = pltpu.roll(z[0], held, 0) + z[0] * flipper
                    imag = pltpu.roll(z[1], held, 0) + z[1] * flipper
                    at = r + 4 * s
                    acc_ref[at] += real * screen_ref[p, at, 0] - imag * screen_ref[p, at, 1]
            return carry

        lax.fori_loop(0, planes, one_plane, 0)
        for at in range(16):
            img_refs[k][pl.ds(at, 8, stride=16), :] = acc_ref[at]

    span = per * 16

    def x_copies(k):
        copies = []
        for d in range(1, n_seat):
            for h in range(2):
                row = pl.multiple_of((held * h + seat_peer(d) * per) * 16, 16)
                copies.append(
                    pltpu.make_async_remote_copy(
                        src_ref=img_refs[k].at[pl.ds(row, span), :], dst_ref=xland_ref.at[k, d, h],
                        send_sem=x_send.at[k, d, h], recv_sem=x_recv.at[k, d, h],
                        device_id=(seat_peer(d) * CORES + core, bl), device_id_type=MESH,
                    )
                )
        return copies

    def b_copies(k):
        return [
            pltpu.make_async_remote_copy(
                src_ref=sum_ref.at[k, bl_peer(d)], dst_ref=bland_ref.at[k, d],
                send_sem=b_send.at[k, d], recv_sem=b_recv.at[k, d],
                device_id=(chan, bl_peer(d)), device_id_type=MESH,
            )
            for d in range(1, n_bl)
        ]

    share = per * NPIX // (n_bl * LANES)

    def gather_x(k, copies):
        for copy in copies:
            copy.wait()
        for h in range(2):
            row = pl.multiple_of((held * h + seat * per) * 16, 16)
            total = img_refs[k][pl.ds(row, span), :]
            for d in range(1, n_seat):
                total = total + xland_ref[k, d, h]
            for i in range(per):
                at = (i * 32 + h * 16) // share
                sum_ref[k, at : at + 16 // share] = total[i * 16 : (i + 1) * 16].reshape(16 // share, share, LANES)
        copies = b_copies(k)
        for copy in copies:
            copy.start()
        return copies

    x_flight = []
    b_flight = []
    for k in range(TAYLOR):
        transform(k)
        x_flight.append(x_copies(k))
        for copy in x_flight[-1]:
            copy.start()
        if k == 0:
            for copy in mom_x:
                copy.wait()
            total = msend_ref[...]
            for d in range(1, n_seat):
                total = total + mxland_ref[d]
            msum_ref[...] = total
            mom_b = [
                pltpu.make_async_remote_copy(
                    src_ref=msum_ref, dst_ref=mbland_ref.at[d], send_sem=bm_send.at[d], recv_sem=bm_recv.at[d],
                    device_id=(chan, bl_peer(d)), device_id_type=MESH,
                )
                for d in range(1, n_bl)
            ]
            for copy in mom_b:
                copy.start()
        else:
            b_flight.append(gather_x(k - 1, x_flight[k - 1]))
    b_flight.append(gather_x(TAYLOR - 1, x_flight[-1]))

    moments = msum_ref[...]
    for d in range(1, n_bl):
        mom_b[d - 1].wait()
        moments = moments + mbland_ref[d]
    images = []
    for k in range(TAYLOR):
        total = sum_ref[k, bl]
        for d in range(1, n_bl):
            b_flight[k][d - 1].wait()
            total = total + bland_ref[k, d]
        images.append(total)
    solved = solve_taylor([moments[m : m + 1] for m in range(MOMENTS)], images)
    for k in range(TAYLOR):
        out_ref[k] = solved[k]


def strip_image(n_chan, n_bl, count, offsets, value, weight, kernel, tiles, plane, chans):
    consts = [jnp.asarray(t) for t in tables(n_chan)]
    tap_table, coarse, twist, screen = consts
    smem = pl.BlockSpec(memory_space=pltpu.SMEM)
    vmem = pl.BlockSpec(memory_space=pltpu.VMEM)
    hbm = pl.BlockSpec(memory_space=pl.ANY)
    slots = kernel.shape[1]
    n_seat = n_chan // CORES
    per = STRIP // n_chan
    share = per * NPIX // (n_bl * LANES)
    f32 = jnp.float32
    bf16 = jnp.bfloat16
    dma = pltpu.SemaphoreType.DMA
    scratch = [
        (tap_table.shape[1:], bf16), (coarse.shape, bf16), (twist.shape, f32), (screen.shape[1:], f32),
        ((8, slots), f32), ((8, slots), f32), (kernel.shape, bf16),
        ((rows_all, BLK), bf16), ((rows_all, BLK), bf16), ((BLK, LANES), f32),
        ((groups, rows_all, 2 * LANES), f32), ((8, BLK), f32), ((planes * quads * 32, 2 * LANES), f32),
        ((16, 8, LANES), f32), ((LANES, LANES), f32), ((LANES, LANES), f32), ((LANES, LANES), f32),
        ((TAYLOR, n_seat, 2, per * 16, LANES), f32),
        ((TAYLOR, n_bl, share, LANES), f32), ((TAYLOR, n_bl, share, LANES), f32),
        ((8, LANES), f32), ((n_seat, 8, LANES), f32), ((8, LANES), f32), ((n_bl, 8, LANES), f32),
    ]
    return pl.pallas_call(
        functools.partial(strip_kernel, n_chan, n_bl),
        out_shape=jax.ShapeDtypeStruct((TAYLOR, share, LANES), f32),
        in_specs=[smem, smem] + [vmem] * 6 + [hbm] * 4,
        out_specs=vmem,
        scratch_shapes=[pltpu.VMEM(shape, kind) for shape, kind in scratch]
        + [
            dma((4,)), dma((2,)), dma((2,)),
            dma((TAYLOR, n_seat, 2)), dma((TAYLOR, n_seat, 2)), dma((n_seat,)), dma((n_seat,)),
            dma((TAYLOR, n_bl)), dma((TAYLOR, n_bl)), dma((n_bl,)), dma((n_bl,)),
        ],
        compiler_params=pltpu.CompilerParams(
            vmem_limit_bytes=56 * 1024 * 1024, collective_id=0, has_side_effects=True
        ),
        name="strip_image",
    )(count, offsets, value, weight, kernel, tiles, plane, chans, *consts)


def solution(mesh):
    n_chan = mesh.shape["chan"]
    n_bl = mesh.shape["bl"]

    def body(vis_value, vis_weight, kernel, tile_index, plane_index, chan_index, chan_offset, counts):
        out = strip_image(
            n_chan, n_bl, counts, chan_offset, vis_value[0, 0], vis_weight[0], kernel[0, 0],
            tile_index[0], plane_index[0], chan_index[0],
        )
        return out.reshape(TAYLOR, -1)

    in_specs = (
        P("chan", "bl", None, None),
        P("chan", "bl", None),
        P("chan", "bl", None, None),
        P("chan", "bl", None),
        P("chan", "bl", None),
        P("chan", "bl", None),
        P("chan", None),
        P("chan", "bl"),
    )
    out_specs = P(None, ("chan", "bl"))
    return jax.shard_map(body, mesh=mesh, in_specs=in_specs, out_specs=out_specs, check_vma=False)
```

```python
import functools

import numpy as np
import jax
import jax.numpy as jnp
from jax import lax
from jax.experimental import pallas as pl
from jax.experimental.pallas import tpu as pltpu
from jax.sharding import PartitionSpec as P

NPIX = 4096
TILE = 8
TAYLOR = 3
MOMENTS = 5
WPLANES = 8
STRIP = 8
LANES = 128
CORES = 2

two_pi = 2.0 * np.pi
w_step = 40.0
ntiles = NPIX // TILE
planes = WPLANES // 2
held = STRIP // CORES
quads = ntiles // LANES
groups = planes * quads // 2
pairs = TILE // 2
per_k = TILE * STRIP + 8
rows_all = TAYLOR * per_k
BLK = 512
MESH = pl.DeviceIdType.MESH


def split(x):
    high = x.astype(jnp.bfloat16)
    low = (x - high.astype(jnp.float32)).astype(jnp.bfloat16)
    return high, low


def cosine_series():
    g = 0.125 - 0.125 * np.cos(np.pi * (np.arange(64) + 0.5) / 64)
    fit = np.polynomial.Polynomial.fit(g, np.cos(two_pi * np.sqrt(g)), 8, domain=[0.0, 0.25])
    return [float(c) for c in fit.convert().coef]


cos_terms = cosine_series()


@functools.cache
def tables(n_chan):
    f32 = np.float32
    bf16 = jnp.bfloat16
    per = STRIP // n_chan

    def two(x):
        x = x.astype(f32)
        high = x.astype(bf16)
        return high, (x - high.astype(f32)).astype(bf16)

    slot = np.arange(held)
    strips = [(slot // per * CORES + core) * per + slot % per for core in range(CORES)]
    sub_e = np.arange(8) // held
    sub_l = np.arange(8) % held

    taps = np.zeros((CORES, 88, 2, TILE, TILE))
    for core in range(CORES):
        offset = strips[core] - STRIP // 2
        angle = two_pi * np.arange(TILE)[None, :] * offset[:, None] / NPIX
        for e in range(TILE + 1):
            for part, wave in enumerate((np.cos(angle), np.sin(angle))):
                if e < TILE:
                    rows = [part * 32 + e // 2 * 8 + e % 2 * held + slot]
                else:
                    rows = [64 + part * 8 + slot, 64 + part * 8 + held + slot]
                for row in rows:
                    if e < TILE:
                        taps[core, row, 0, :, e] = wave
                    if e > 0:
                        taps[core, row, 1, :, TILE - e] = wave
    taps[:, 80:] = 1.0
    tap_high, tap_low = two(taps.reshape(CORES, 88, 2 * TILE * TILE))
    tap_table = np.concatenate([tap_high, tap_low], axis=2)

    ids = np.arange(LANES)
    angle = two_pi * (ids[:, None] * ids[None, :] % LANES) / LANES
    cosine, sine = np.cos(angle), np.sin(angle)
    coarse = np.stack(two(np.block([[cosine, sine], [-sine, cosine]])))

    cell = (8 * np.arange(quads)[:, None, None] + 2 * np.arange(pairs)[None, :, None] + sub_e[None, None, :])[..., None]
    angle = two_pi * cell * ids / NPIX
    sign = 1.0 - 2.0 * ((cell + ids) % 2)
    twist = np.stack([np.cos(angle) * sign, np.sin(angle) * sign], axis=2)
    e = 2 * np.arange(pairs)[None, :, None] + sub_e[None, None, :]
    angle = np.broadcast_to(two_pi * (np.arange(4)[:, None, None] * e)[..., None] / 32, (4, pairs, 8, LANES))
    inner = np.stack([np.cos(angle), np.sin(angle)], axis=2)
    twist = np.stack([twist, inner]).astype(f32)

    cell_size = 0.5 / NPIX
    screens = []
    for core in range(CORES):
        x = (strips[core][sub_l] - STRIP // 2) * cell_size
        column = ids[None, None, :] + LANES * (np.arange(16)[:, None, None] + 16 * sub_e[None, :, None])
        y = (column - NPIX // 2) * cell_size
        radius = x[None, :, None] ** 2 + y**2
        lowered = -radius / (1.0 + np.sqrt(1.0 - radius))
        w = w_step * (np.arange(planes) - 0.5 * (WPLANES - 1))
        angle = two_pi * w[:, None, None, None] * lowered[None]
        screens.append(np.stack([np.cos(angle), np.sin(angle)], axis=2))
    screen = np.stack(screens).astype(f32)
    return tap_table, coarse, twist, screen


def solve_taylor(moments, images):
    entry_00, entry_01, entry_02 = (moments[0], moments[1], moments[2])
    entry_11, entry_12, entry_22 = (moments[2], moments[3], moments[4])
    minor_00 = entry_11 * entry_22 - entry_12 * entry_12
    minor_01 = entry_02 * entry_12 - entry_01 * entry_22
    minor_02 = entry_01 * entry_12 - entry_02 * entry_11
    minor_11 = entry_00 * entry_22 - entry_02 * entry_02
    minor_12 = entry_01 * entry_02 - entry_00 * entry_12
    minor_22 = entry_00 * entry_11 - entry_01 * entry_01
    determinant = entry_00 * minor_00 + entry_01 * minor_01 + entry_02 * minor_02
    first = (minor_00 * images[0] + minor_01 * images[1] + minor_02 * images[2]) / determinant
    second = (minor_01 * images[0] + minor_11 * images[1] + minor_12 * images[2]) / determinant
    third = (minor_02 * images[0] + minor_12 * images[1] + minor_22 * images[2]) / determinant
    return first, second, third


def multiply(a, b):
    return a[0] * b[0] - a[1] * b[1], a[0] * b[1] + a[1] * b[0]


def radix4(x):
    a = (x[0][0] + x[2][0], x[0][1] + x[2][1])
    b = (x[0][0] - x[2][0], x[0][1] - x[2][1])
    c = (x[1][0] + x[3][0], x[1][1] + x[3][1])
    d = (x[1][0] - x[3][0], x[1][1] - x[3][1])
    return (
        (a[0] + c[0], a[1] + c[1]), (b[0] - d[1], b[1] + d[0]),
        (a[0] - c[0], a[1] - c[1]), (b[0] + d[1], b[1] - d[0]),
    )


def strip_kernel(
    n_chan, n_bl, count_hbm, offset_hbm, value_hbm, weight_hbm, kernel_hbm, tile_hbm, plane_hbm, chan_hbm,
    tap_hbm, coarse_hbm, twist_hbm, screen_hbm, out_ref,
    count_ref, offset_ref, value_ref, weight_ref, kernel_ref, tile_ref, plane_ref, chan_ref,
    tap_ref, coarse_ref, twist_ref, screen_ref, meta_ref, meta_land, taps_land,
    high0_ref, low0_ref, code0_ref, high1_ref, low1_ref, code1_ref,
    grid_ref, mom_ref, spec_ref, acc_ref, img0_ref, img1_ref, img2_ref,
    xland_ref, sum_ref, bland_ref, msend_ref, mland_ref,
    load_sem, pair_send, pair_recv, x_send, x_recv, m_send, m_recv, b_send, b_recv,
):
    chan = lax.axis_index("chan")
    bl = lax.axis_index("bl")
    core = lax.rem(chan, CORES)
    seat = chan // CORES
    n_seat = n_chan // CORES
    per = STRIP // n_chan
    img_refs = (img0_ref, img1_ref, img2_ref)
    slots = kernel_ref.shape[1]

    def seat_peer(d):
        return lax.rem(seat + d, n_seat)

    def bl_peer(d):
        return lax.rem(bl + d, n_bl)

    mate = (chan + 1 - 2 * core, bl)
    loads = [
        pltpu.make_async_copy(source, target, load_sem.at[i])
        for i, (source, target) in enumerate((
            (count_hbm, count_ref), (offset_hbm, offset_ref), (value_hbm, value_ref), (weight_hbm, weight_ref),
            (tile_hbm, tile_ref), (plane_hbm, plane_ref), (chan_hbm, chan_ref),
            (kernel_hbm, kernel_ref), (tap_hbm.at[core], tap_ref), (coarse_hbm, coarse_ref),
            (twist_hbm, twist_ref), (screen_hbm.at[core], screen_ref),
        ))
    ]
    for load in loads:
        load.start()

    barrier = pltpu.get_barrier_semaphore()
    pl.semaphore_signal(barrier, inc=1, device_id=mate, device_id_type=MESH)
    peers = [(a, d) for a in range(n_seat) for d in range(n_bl) if a or d]
    for a, d in peers:
        pl.semaphore_signal(
            barrier, inc=1, device_id=(seat_peer(a) * CORES + core, bl_peer(d)), device_id_type=MESH
        )

    mom_ref[...] = jnp.zeros_like(mom_ref)
    for load in loads[:7]:
        load.wait()

    slot = lax.broadcasted_iota(jnp.int32, (1, slots), 1)
    tiles = tile_ref[...]
    plane = plane_ref[...]
    chans = chan_ref[...]
    coord = jnp.zeros((1, slots), jnp.float32)
    for c in range(offset_ref.shape[1]):
        coord = jnp.where(chans == c, offset_ref[0:1, c : c + 1], coord)
    weight = jnp.where(slot < count_ref[...], weight_ref[...].astype(jnp.float32), 0.0)
    value = value_ref[...].astype(jnp.float32)
    flip = plane >= planes
    v_tile = tiles & (ntiles - 1)
    v_tile = jnp.where(flip, ntiles - 1 - v_tile, v_tile)
    fold = jnp.where(flip, WPLANES - 1 - plane, plane)
    place = (fold * quads + (v_tile & (quads - 1))) * LANES + lax.shift_right_logical(v_tile, quads.bit_length() - 1)
    meta_ref[0:1, :] = weight * value[0:1]
    meta_ref[1:2, :] = weight * value[1:2]
    meta_ref[2:3, :] = coord
    meta_ref[3:4, :] = weight
    meta_ref[4:5, :] = (lax.shift_right_logical(tiles, ntiles.bit_length() - 1) - ntiles // 2).astype(jnp.float32)
    meta_ref[5:6, :] = place.astype(jnp.float32)
    meta_ref[6:7, :] = jnp.where(flip, -1.0, 1.0)
    meta_ref[7:8, :] = jnp.zeros((1, slots), jnp.float32)

    sub = lax.broadcasted_iota(jnp.int32, (8, 1), 0)
    first = sub < held
    local = lax.rem(sub, held)
    strip = (local // per * CORES + core) * per + lax.rem(local, per) - STRIP // 2
    turn = strip.astype(jnp.float32) * (1.0 / ntiles)
    quarter = jnp.where(first, 0.0, 0.25)

    for load in loads[7:9]:
        load.wait()

    buffers = ((high0_ref, low0_ref, code0_ref), (high1_ref, low1_ref, code1_ref))

    def prepare(taps_ref, rows_ref, block, buffer):
        high_ref, low_ref, code_ref = buffer
        here = pl.ds(block * BLK, BLK)
        base_real = rows_ref[0:1, here]
        base_imag = rows_ref[1:2, here]
        coord = rows_ref[2:3, here]
        weight = rows_ref[3:4, here]
        u_off = rows_ref[4:5, here]
        place = rows_ref[5:6, here]
        sign = rows_ref[6:7, here]
        taps = taps_ref[:, here]
        plain = taps * jnp.maximum(sign, 0.0).astype(jnp.bfloat16)
        turned = taps * jnp.maximum(-sign, 0.0).astype(jnp.bfloat16)
        sums = jnp.dot(
            tap_ref[...], jnp.concatenate([plain, turned, plain, turned], axis=0),
            preferred_element_type=jnp.float32,
        )
        cycle = u_off * turn - quarter
        cycle = cycle - jnp.floor(cycle + 0.5)
        square = cycle * cycle
        wave = jnp.full_like(square, cos_terms[-1])
        for term in cos_terms[-2::-1]:
            wave = wave * square + term
        other = pltpu.roll(wave, held, 0)
        cosine = jnp.where(first, wave, other)
        sine = jnp.where(first, other, wave)
        z_real = base_real * cosine - base_imag * sine
        z_imag = base_real * sine + base_imag * cosine
        s_real = z_real * sign
        s_imag = z_imag * sign
        sum_real = sums[0:32].reshape(pairs, 8, BLK)
        sum_imag = sums[32:64].reshape(pairs, 8, BLK)
        part_real = (sum_real * z_real[None] - sum_imag * z_imag[None]).reshape(32, BLK)
        part_imag = (sum_real * s_imag[None] + sum_imag * s_real[None]).reshape(32, BLK)
        edge = sums[64:72] * jnp.where(first, z_real, s_imag) + sums[72:80] * jnp.where(first, -z_imag, s_real)
        part = jnp.concatenate([part_real, part_imag, edge], axis=0)
        parts = [part]
        for k in range(1, TAYLOR):
            parts.append(parts[-1] * coord)
        high, low = split(jnp.concatenate(parts, axis=0))
        high_ref[...] = high
        low_ref[...] = low

        weighted = weight * sums[80:81]
        power = weighted
        for m in range(MOMENTS):
            mom_ref[m : m + 1, :] += power
            power = power * coord

        lane = lax.broadcasted_iota(jnp.int32, (BLK, LANES), 1).astype(jnp.float32)
        column = jnp.transpose(jnp.broadcast_to(place, (LANES, BLK)))
        level = (column - lane) * (1.0 / LANES)
        code_ref[...] = jnp.where(jnp.floor(level) == level, level, -1.0).astype(jnp.bfloat16)

    def scatter(buffer, fresh):
        high_ref, low_ref, code_ref = buffer
        one = jnp.bfloat16(1.0)
        zero = jnp.bfloat16(0.0)
        for g in range(groups):
            hot = jnp.concatenate(
                [jnp.where(code_ref[...] == jnp.bfloat16(2 * g + h), one, zero) for h in range(2)], axis=1
            )
            update = jnp.dot(high_ref[...], hot, preferred_element_type=jnp.float32) + jnp.dot(
                low_ref[...], hot, preferred_element_type=jnp.float32
            )
            if fresh:
                grid_ref[g] = update
            else:
                grid_ref[g] += update

    blocks = slots // BLK
    swaps = [
        pltpu.make_async_remote_copy(
            src_ref=source, dst_ref=target, send_sem=pair_send.at[i], recv_sem=pair_recv.at[i],
            device_id=mate, device_id_type=MESH,
        )
        for i, (source, target) in enumerate(((kernel_ref, taps_land), (meta_ref, meta_land)))
    ]
    order = [(kernel_ref, meta_ref, j) for j in range(blocks)] + [(taps_land, meta_land, j) for j in range(blocks)]
    prepare(*order[0], buffers[0])
    for j in range(2 * blocks):
        if j == blocks // 2:
            pl.semaphore_wait(barrier, 1 + n_seat * n_bl - 1)
            for swap in swaps:
                swap.start()
        if j + 1 == blocks:
            for swap in swaps:
                swap.wait()
        if j + 1 < 2 * blocks:
            prepare(*order[j + 1], buffers[(j + 1) % 2])
        scatter(buffers[j % 2], j == 0)

    msend_ref[...] = jnp.broadcast_to(jnp.sum(mom_ref[...], axis=1, keepdims=True), msend_ref.shape)
    mom_copies = [
        pltpu.make_async_remote_copy(
            src_ref=msend_ref, dst_ref=mland_ref.at[i], send_sem=m_send.at[i], recv_sem=m_recv.at[i],
            device_id=(seat_peer(a) * CORES + core, bl_peer(d)), device_id_type=MESH,
        )
        for i, (a, d) in enumerate(peers)
    ]
    for copy in mom_copies:
        copy.start()

    for load in loads[9:]:
        load.wait()
    flipper = jnp.where(first, 1.0, -1.0)
    spin = [
        (jnp.where(first, 1.0, float(np.cos(two_pi * s / 8))), jnp.where(first, 0.0, float(np.sin(two_pi * s / 8))))
        for s in range(4)
    ]

    def transform(k):
        low_row = k * per_k
        pieces = []
        for p in range(planes):
            edges = []
            for b in range(quads):
                q = p * quads + b
                lanes = pl.ds(q % 2 * LANES, LANES)
                edges.append(grid_ref[q // 2, low_row + 64 : low_row + 72, lanes])
            edges = [pltpu.roll(edges[-1], 1, 1)] + edges[:-1]
            for b in range(quads):
                q = p * quads + b
                lanes = pl.ds(q % 2 * LANES, LANES)
                real = grid_ref[q // 2, low_row : low_row + 32, lanes]
                imag = grid_ref[q // 2, low_row + 32 : low_row + 64, lanes]
                edge = edges[b]
                head_real = real[:8] + jnp.where(first, edge, 0.0)
                head_imag = imag[:8] + jnp.where(first, pltpu.roll(edge, held, 0), 0.0)
                real = jnp.concatenate([head_real, real[8:]], axis=0)
                imag = jnp.concatenate([head_imag, imag[8:]], axis=0)
                pieces.append(jnp.concatenate([real, imag], axis=1))
        high, low = split(jnp.concatenate(pieces, axis=0))
        spec_ref[...] = (
            jnp.dot(high, coarse_ref[0], preferred_element_type=jnp.float32)
            + jnp.dot(high, coarse_ref[1], preferred_element_type=jnp.float32)
            + jnp.dot(low, coarse_ref[0], preferred_element_type=jnp.float32)
        )
        acc_ref[...] = jnp.zeros_like(acc_ref)

        def one_plane(p, carry):
            inner = [[None] * pairs for r in range(4)]
            for t in range(pairs):
                column = []
                for b in range(quads):
                    row = pl.ds(pl.multiple_of((p * quads + b) * 32 + t * 8, 8), 8)
                    x = (spec_ref[row, :LANES], spec_ref[row, LANES:])
                    column.append(multiply(x, (twist_ref[0, b, t, 0], twist_ref[0, b, t, 1])))
                for r, z in enumerate(radix4(column)):
                    inner[r][t] = multiply(z, (twist_ref[1, r, t, 0], twist_ref[1, r, t, 1])) if r else z
            for r in range(4):
                for s, z in enumerate(radix4(inner[r])):
                    if s:
                        z = multiply(z, spin[s])
                    real = pltpu.roll(z[0], held, 0) + z[0] * flipper
                    imag = pltpu.roll(z[1], held, 0) + z[1] * flipper
                    at = r + 4 * s
                    acc_ref[at] += real * screen_ref[p, at, 0] - imag * screen_ref[p, at, 1]
            return carry

        lax.fori_loop(0, planes, one_plane, 0)
        for at in range(16):
            img_refs[k][pl.ds(at, 8, stride=16), :] = acc_ref[at]

    span = per * 16

    def x_copies(k):
        copies = []
        for d in range(1, n_seat):
            for h in range(2):
                row = pl.multiple_of((held * h + seat_peer(d) * per) * 16, 16)
                copies.append(
                    pltpu.make_async_remote_copy(
                        src_ref=img_refs[k].at[pl.ds(row, span), :], dst_ref=xland_ref.at[k, d, h],
                        send_sem=x_send.at[k, d, h], recv_sem=x_recv.at[k, d, h],
                        device_id=(seat_peer(d) * CORES + core, bl), device_id_type=MESH,
                    )
                )
        return copies

    def b_copies(k):
        return [
            pltpu.make_async_remote_copy(
                src_ref=sum_ref.at[k, bl_peer(d)], dst_ref=bland_ref.at[k, d],
                send_sem=b_send.at[k, d], recv_sem=b_recv.at[k, d],
                device_id=(chan, bl_peer(d)), device_id_type=MESH,
            )
            for d in range(1, n_bl)
        ]

    share = per * NPIX // (n_bl * LANES)

    def gather_x(k, copies):
        for copy in copies:
            copy.wait()
        for h in range(2):
            row = pl.multiple_of((held * h + seat * per) * 16, 16)
            total = img_refs[k][pl.ds(row, span), :]
            for d in range(1, n_seat):
                total = total + xland_ref[k, d, h]
            for i in range(per):
                at = (i * 32 + h * 16) // share
                sum_ref[k, at : at + 16 // share] = total[i * 16 : (i + 1) * 16].reshape(16 // share, share, LANES)
        copies = b_copies(k)
        for copy in copies:
            copy.start()
        return copies

    x_flight = []
    b_flight = []
    for k in range(TAYLOR):
        transform(k)
        x_flight.append(x_copies(k))
        for copy in x_flight[-1]:
            copy.start()
    for k in range(TAYLOR):
        b_flight.append(gather_x(k, x_flight[k]))

    moments = msend_ref[...]
    for i, copy in enumerate(mom_copies):
        copy.wait()
        moments = moments + mland_ref[i]
    images = []
    for k in range(TAYLOR):
        total = sum_ref[k, bl]
        for d in range(1, n_bl):
            b_flight[k][d - 1].wait()
            total = total + bland_ref[k, d]
        images.append(total)
    solved = solve_taylor([moments[m : m + 1] for m in range(MOMENTS)], images)
    for k in range(TAYLOR):
        out_ref[k] = solved[k]


def strip_image(n_chan, n_bl, count, offsets, value, weight, kernel, tiles, plane, chans):
    consts = [jnp.asarray(t) for t in tables(n_chan)]
    tap_table, coarse, twist, screen = consts
    vmem = pl.BlockSpec(memory_space=pltpu.VMEM)
    hbm = pl.BlockSpec(memory_space=pl.ANY)
    slots = kernel.shape[1]
    n_seat = n_chan // CORES
    per = STRIP // n_chan
    share = per * NPIX // (n_bl * LANES)
    f32 = jnp.float32
    bf16 = jnp.bfloat16
    dma = pltpu.SemaphoreType.DMA
    block = [((rows_all, BLK), bf16), ((rows_all, BLK), bf16), ((BLK, LANES), bf16)]
    inputs = (count, offsets, value, weight, kernel, tiles, plane, chans)
    peers = n_seat * n_bl - 1
    scratch = [(x.shape, x.dtype) for x in inputs] + [
        (tap_table.shape[1:], bf16), (coarse.shape, bf16), (twist.shape, f32), (screen.shape[1:], f32),
        ((8, slots), f32), ((8, slots), f32), (kernel.shape, bf16),
        *block, *block,
        ((groups, rows_all, 2 * LANES), f32), ((8, BLK), f32), ((planes * quads * 32, 2 * LANES), f32),
        ((16, 8, LANES), f32), ((LANES, LANES), f32), ((LANES, LANES), f32), ((LANES, LANES), f32),
        ((TAYLOR, n_seat, 2, per * 16, LANES), f32),
        ((TAYLOR, n_bl, share, LANES), f32), ((TAYLOR, n_bl, share, LANES), f32),
        ((8, LANES), f32), ((peers, 8, LANES), f32),
    ]
    return pl.pallas_call(
        functools.partial(strip_kernel, n_chan, n_bl),
        out_shape=jax.ShapeDtypeStruct((TAYLOR, share, LANES), f32),
        in_specs=[hbm] * (len(inputs) + len(consts)),
        out_specs=vmem,
        scratch_shapes=[pltpu.VMEM(shape, kind) for shape, kind in scratch]
        + [
            dma((len(inputs) + len(consts),)), dma((2,)), dma((2,)),
            dma((TAYLOR, n_seat, 2)), dma((TAYLOR, n_seat, 2)), dma((peers,)), dma((peers,)),
            dma((TAYLOR, n_bl)), dma((TAYLOR, n_bl)),
        ],
        compiler_params=pltpu.CompilerParams(
            vmem_limit_bytes=56 * 1024 * 1024, collective_id=0, has_side_effects=True
        ),
        name="strip_image",
    )(*inputs, *consts)


def solution(mesh):
    n_chan = mesh.shape["chan"]
    n_bl = mesh.shape["bl"]

    def body(vis_value, vis_weight, kernel, tile_index, plane_index, chan_index, chan_offset, counts):
        out = strip_image(
            n_chan, n_bl, counts, chan_offset, vis_value[0, 0], vis_weight[0], kernel[0, 0],
            tile_index[0], plane_index[0], chan_index[0],
        )
        return out.reshape(TAYLOR, -1)

    in_specs = (
        P("chan", "bl", None, None),
        P("chan", "bl", None),
        P("chan", "bl", None, None),
        P("chan", "bl", None),
        P("chan", "bl", None),
        P("chan", "bl", None),
        P("chan", None),
        P("chan", "bl"),
    )
    out_specs = P(None, ("chan", "bl"))
    return jax.shard_map(body, mesh=mesh, in_specs=in_specs, out_specs=out_specs, check_vma=False)
```

```python
import functools

import numpy as np
import jax
import jax.numpy as jnp
from jax import lax
from jax.experimental import pallas as pl
from jax.experimental.pallas import tpu as pltpu
from jax.sharding import PartitionSpec as P

NPIX = 4096
TILE = 8
TAYLOR = 3
MOMENTS = 5
WPLANES = 8
STRIP = 8
LANES = 128
CORES = 2

two_pi = 2.0 * np.pi
w_step = 40.0
ntiles = NPIX // TILE
planes = WPLANES // 2
held = STRIP // CORES
quads = ntiles // LANES
groups = planes * quads // 2
pairs = TILE // 2
per_k = TILE * STRIP + 8
rows_all = TAYLOR * per_k
BLK = 512
MESH = pl.DeviceIdType.MESH


def split(x):
    high = x.astype(jnp.bfloat16)
    low = (x - high.astype(jnp.float32)).astype(jnp.bfloat16)
    return high, low


def cosine_series():
    g = 0.125 - 0.125 * np.cos(np.pi * (np.arange(64) + 0.5) / 64)
    fit = np.polynomial.Polynomial.fit(g, np.cos(two_pi * np.sqrt(g)), 8, domain=[0.0, 0.25])
    return [float(c) for c in fit.convert().coef]


cos_terms = cosine_series()


@functools.cache
def tables(n_chan):
    f32 = np.float32
    bf16 = jnp.bfloat16
    per = STRIP // n_chan

    def two(x):
        x = x.astype(f32)
        high = x.astype(bf16)
        return high, (x - high.astype(f32)).astype(bf16)

    slot = np.arange(held)
    strips = [(slot // per * CORES + core) * per + slot % per for core in range(CORES)]
    sub_e = np.arange(8) // held
    sub_l = np.arange(8) % held

    taps = np.zeros((CORES, 88, 2, TILE, TILE))
    for core in range(CORES):
        offset = strips[core] - STRIP // 2
        angle = two_pi * np.arange(TILE)[None, :] * offset[:, None] / NPIX
        for e in range(TILE + 1):
            for part, wave in enumerate((np.cos(angle), np.sin(angle))):
                if e < TILE:
                    rows = [part * 32 + e // 2 * 8 + e % 2 * held + slot]
                else:
                    rows = [64 + part * 8 + slot, 64 + part * 8 + held + slot]
                for row in rows:
                    if e < TILE:
                        taps[core, row, 0, :, e] = wave
                    if e > 0:
                        taps[core, row, 1, :, TILE - e] = wave
    taps[:, 80:] = 1.0
    tap_high, tap_low = two(taps.reshape(CORES, 88, 2 * TILE * TILE))
    tap_table = np.concatenate([tap_high, tap_low], axis=2)

    ids = np.arange(LANES)
    angle = two_pi * (ids[:, None] * ids[None, :] % LANES) / LANES
    cosine, sine = np.cos(angle), np.sin(angle)
    coarse = np.stack(two(np.block([[cosine, sine], [-sine, cosine]])))

    cell = (8 * np.arange(quads)[:, None, None] + 2 * np.arange(pairs)[None, :, None] + sub_e[None, None, :])[..., None]
    angle = two_pi * cell * ids / NPIX
    sign = 1.0 - 2.0 * ((cell + ids) % 2)
    twist = np.stack([np.cos(angle) * sign, np.sin(angle) * sign], axis=2)
    e = 2 * np.arange(pairs)[None, :, None] + sub_e[None, None, :]
    angle = np.broadcast_to(two_pi * (np.arange(4)[:, None, None] * e)[..., None] / 32, (4, pairs, 8, LANES))
    inner = np.stack([np.cos(angle), np.sin(angle)], axis=2)
    twist = np.stack([twist, inner]).astype(f32)

    cell_size = 0.5 / NPIX
    screens = []
    for core in range(CORES):
        x = (strips[core][sub_l] - STRIP // 2) * cell_size
        column = ids[None, None, :] + LANES * (np.arange(16)[:, None, None] + 16 * sub_e[None, :, None])
        y = (column - NPIX // 2) * cell_size
        radius = x[None, :, None] ** 2 + y**2
        lowered = -radius / (1.0 + np.sqrt(1.0 - radius))
        w = w_step * (np.arange(planes) - 0.5 * (WPLANES - 1))
        angle = two_pi * w[:, None, None, None] * lowered[None]
        screens.append(np.stack([np.cos(angle), np.sin(angle)], axis=2))
    screen = np.stack(screens).astype(f32)
    return tap_table, coarse, twist, screen


def solve_taylor(moments, images):
    entry_00, entry_01, entry_02 = (moments[0], moments[1], moments[2])
    entry_11, entry_12, entry_22 = (moments[2], moments[3], moments[4])
    minor_00 = entry_11 * entry_22 - entry_12 * entry_12
    minor_01 = entry_02 * entry_12 - entry_01 * entry_22
    minor_02 = entry_01 * entry_12 - entry_02 * entry_11
    minor_11 = entry_00 * entry_22 - entry_02 * entry_02
    minor_12 = entry_01 * entry_02 - entry_00 * entry_12
    minor_22 = entry_00 * entry_11 - entry_01 * entry_01
    determinant = entry_00 * minor_00 + entry_01 * minor_01 + entry_02 * minor_02
    first = (minor_00 * images[0] + minor_01 * images[1] + minor_02 * images[2]) / determinant
    second = (minor_01 * images[0] + minor_11 * images[1] + minor_12 * images[2]) / determinant
    third = (minor_02 * images[0] + minor_12 * images[1] + minor_22 * images[2]) / determinant
    return first, second, third


def multiply(a, b):
    return a[0] * b[0] - a[1] * b[1], a[0] * b[1] + a[1] * b[0]


def radix4(x):
    a = (x[0][0] + x[2][0], x[0][1] + x[2][1])
    b = (x[0][0] - x[2][0], x[0][1] - x[2][1])
    c = (x[1][0] + x[3][0], x[1][1] + x[3][1])
    d = (x[1][0] - x[3][0], x[1][1] - x[3][1])
    return (
        (a[0] + c[0], a[1] + c[1]), (b[0] - d[1], b[1] + d[0]),
        (a[0] - c[0], a[1] - c[1]), (b[0] + d[1], b[1] - d[0]),
    )


def strip_kernel(
    n_chan, n_bl, count_hbm, offset_hbm, value_hbm, weight_hbm, kernel_hbm, tile_hbm, plane_hbm, chan_hbm,
    tap_hbm, coarse_hbm, twist_hbm, screen_hbm, out_ref,
    count_ref, offset_ref, value_ref, weight_ref, kernel_ref, tile_ref, plane_ref, chan_ref,
    tap_ref, coarse_ref, twist_ref, screen_ref, meta_ref, meta_land, taps_land,
    high0_ref, low0_ref, code0_ref, high1_ref, low1_ref, code1_ref,
    grid_ref, mom_ref, spec_ref, acc_ref, img0_ref, img1_ref, img2_ref,
    xland_ref, sum_ref, bland_ref, msend_ref, mland_ref,
    load_sem, pair_send, pair_recv, x_send, x_recv, m_send, m_recv, b_send, b_recv,
):
    chan = lax.axis_index("chan")
    bl = lax.axis_index("bl")
    core = lax.rem(chan, CORES)
    seat = chan // CORES
    n_seat = n_chan // CORES
    per = STRIP // n_chan
    img_refs = (img0_ref, img1_ref, img2_ref)
    slots = kernel_ref.shape[1]

    def seat_peer(d):
        return lax.rem(seat + d, n_seat)

    def bl_peer(d):
        return lax.rem(bl + d, n_bl)

    mate = (chan + 1 - 2 * core, bl)
    loads = [
        pltpu.make_async_copy(source, target, load_sem.at[i])
        for i, (source, target) in enumerate((
            (count_hbm, count_ref), (offset_hbm, offset_ref), (value_hbm, value_ref), (weight_hbm, weight_ref),
            (tile_hbm, tile_ref), (plane_hbm, plane_ref), (chan_hbm, chan_ref),
            (kernel_hbm, kernel_ref), (tap_hbm.at[core], tap_ref), (coarse_hbm, coarse_ref),
            (twist_hbm, twist_ref), (screen_hbm.at[core], screen_ref),
        ))
    ]
    for load in loads:
        load.start()

    barrier = pltpu.get_barrier_semaphore()
    pl.semaphore_signal(barrier, inc=1, device_id=mate, device_id_type=MESH)
    peers = [(a, d) for a in range(n_seat) for d in range(n_bl) if a or d]
    for a, d in peers:
        pl.semaphore_signal(
            barrier, inc=1, device_id=(seat_peer(a) * CORES + core, bl_peer(d)), device_id_type=MESH
        )

    mom_ref[...] = jnp.zeros_like(mom_ref)
    for load in loads[:7]:
        load.wait()

    slot = lax.broadcasted_iota(jnp.int32, (1, slots), 1)
    tiles = tile_ref[...]
    plane = plane_ref[...]
    chans = chan_ref[...]
    coord = jnp.zeros((1, slots), jnp.float32)
    for c in range(offset_ref.shape[1]):
        coord = jnp.where(chans == c, offset_ref[0:1, c : c + 1], coord)
    weight = jnp.where(slot < count_ref[...], weight_ref[...].astype(jnp.float32), 0.0)
    value = value_ref[...].astype(jnp.float32)
    flip = plane >= planes
    v_tile = tiles & (ntiles - 1)
    v_tile = jnp.where(flip, ntiles - 1 - v_tile, v_tile)
    fold = jnp.where(flip, WPLANES - 1 - plane, plane)
    place = (fold * quads + (v_tile & (quads - 1))) * LANES + lax.shift_right_logical(v_tile, quads.bit_length() - 1)
    meta_ref[0:1, :] = weight * value[0:1]
    meta_ref[1:2, :] = weight * value[1:2]
    meta_ref[2:3, :] = coord
    meta_ref[3:4, :] = weight
    meta_ref[4:5, :] = (lax.shift_right_logical(tiles, ntiles.bit_length() - 1) - ntiles // 2).astype(jnp.float32)
    meta_ref[5:6, :] = place.astype(jnp.float32)
    meta_ref[6:7, :] = jnp.where(flip, -1.0, 1.0)
    meta_ref[7:8, :] = jnp.zeros((1, slots), jnp.float32)

    sub = lax.broadcasted_iota(jnp.int32, (8, 1), 0)
    first = sub < held
    local = lax.rem(sub, held)
    strip = (local // per * CORES + core) * per + lax.rem(local, per) - STRIP // 2
    turn = strip.astype(jnp.float32) * (1.0 / ntiles)
    quarter = jnp.where(first, 0.0, 0.25)

    for load in loads[7:9]:
        load.wait()

    buffers = ((high0_ref, low0_ref, code0_ref), (high1_ref, low1_ref, code1_ref))

    def prepare(taps_ref, rows_ref, block, buffer):
        high_ref, low_ref, code_ref = buffer
        here = pl.ds(block * BLK, BLK)
        base_real = rows_ref[0:1, here]
        base_imag = rows_ref[1:2, here]
        coord = rows_ref[2:3, here]
        weight = rows_ref[3:4, here]
        u_off = rows_ref[4:5, here]
        place = rows_ref[5:6, here]
        sign = rows_ref[6:7, here]
        taps = taps_ref[:, here]
        plain = taps * jnp.maximum(sign, 0.0).astype(jnp.bfloat16)
        turned = taps * jnp.maximum(-sign, 0.0).astype(jnp.bfloat16)
        sums = jnp.dot(
            tap_ref[...], jnp.concatenate([plain, turned, plain, turned], axis=0),
            preferred_element_type=jnp.float32,
        )
        cycle = u_off * turn - quarter
        cycle = cycle - jnp.floor(cycle + 0.5)
        square = cycle * cycle
        wave = jnp.full_like(square, cos_terms[-1])
        for term in cos_terms[-2::-1]:
            wave = wave * square + term
        other = pltpu.roll(wave, held, 0)
        cosine = jnp.where(first, wave, other)
        sine = jnp.where(first, other, wave)
        z_real = base_real * cosine - base_imag * sine
        z_imag = base_real * sine + base_imag * cosine
        s_real = z_real * sign
        s_imag = z_imag * sign
        sum_real = sums[0:32].reshape(pairs, 8, BLK)
        sum_imag = sums[32:64].reshape(pairs, 8, BLK)
        part_real = (sum_real * z_real[None] - sum_imag * z_imag[None]).reshape(32, BLK)
        part_imag = (sum_real * s_imag[None] + sum_imag * s_real[None]).reshape(32, BLK)
        edge = sums[64:72] * jnp.where(first, z_real, s_imag) + sums[72:80] * jnp.where(first, -z_imag, s_real)
        part = jnp.concatenate([part_real, part_imag, edge], axis=0)
        parts = [part]
        for k in range(1, TAYLOR):
            parts.append(parts[-1] * coord)
        high, low = split(jnp.concatenate(parts, axis=0))
        high_ref[...] = high
        low_ref[...] = low

        weighted = weight * sums[80:81]
        power = weighted
        for m in range(MOMENTS):
            mom_ref[m : m + 1, :] += power
            power = power * coord

        lane = lax.broadcasted_iota(jnp.int32, (BLK, LANES), 1).astype(jnp.float32)
        column = jnp.transpose(jnp.broadcast_to(place, (LANES, BLK)))
        level = (column - lane) * (1.0 / LANES)
        code_ref[...] = jnp.where(jnp.floor(level) == level, level, -1.0).astype(jnp.bfloat16)

    def scatter(buffer, fresh):
        high_ref, low_ref, code_ref = buffer
        one = jnp.bfloat16(1.0)
        zero = jnp.bfloat16(0.0)
        for g in range(groups):
            hot = jnp.concatenate(
                [jnp.where(code_ref[...] == jnp.bfloat16(2 * g + h), one, zero) for h in range(2)], axis=1
            )
            update = jnp.dot(high_ref[...], hot, preferred_element_type=jnp.float32) + jnp.dot(
                low_ref[...], hot, preferred_element_type=jnp.float32
            )
            if fresh:
                grid_ref[g] = update
            else:
                grid_ref[g] += update

    blocks = slots // BLK
    swaps = [
        pltpu.make_async_remote_copy(
            src_ref=source, dst_ref=target, send_sem=pair_send.at[i], recv_sem=pair_recv.at[i],
            device_id=mate, device_id_type=MESH,
        )
        for i, (source, target) in enumerate(((kernel_ref, taps_land), (meta_ref, meta_land)))
    ]
    order = [(kernel_ref, meta_ref, j) for j in range(blocks)] + [(taps_land, meta_land, j) for j in range(blocks)]
    prepare(*order[0], buffers[0])
    for j in range(2 * blocks):
        if j == 1:
            pl.semaphore_wait(barrier, 1 + n_seat * n_bl - 1)
            for swap in swaps:
                swap.start()
        if j + 1 == blocks:
            for swap in swaps:
                swap.wait()
        if j + 1 < 2 * blocks:
            prepare(*order[j + 1], buffers[(j + 1) % 2])
        scatter(buffers[j % 2], j == 0)

    msend_ref[...] = jnp.broadcast_to(jnp.sum(mom_ref[...], axis=1, keepdims=True), msend_ref.shape)
    mom_copies = [
        pltpu.make_async_remote_copy(
            src_ref=msend_ref, dst_ref=mland_ref.at[i], send_sem=m_send.at[i], recv_sem=m_recv.at[i],
            device_id=(seat_peer(a) * CORES + core, bl_peer(d)), device_id_type=MESH,
        )
        for i, (a, d) in enumerate(peers)
    ]
    for copy in mom_copies:
        copy.start()

    for load in loads[9:]:
        load.wait()
    flipper = jnp.where(first, 1.0, -1.0)
    spin = [
        (jnp.where(first, 1.0, float(np.cos(two_pi * s / 8))), jnp.where(first, 0.0, float(np.sin(two_pi * s / 8))))
        for s in range(4)
    ]

    def transform(k):
        low_row = k * per_k
        pieces = []
        for p in range(planes):
            edges = []
            for b in range(quads):
                q = p * quads + b
                lanes = pl.ds(q % 2 * LANES, LANES)
                edges.append(grid_ref[q // 2, low_row + 64 : low_row + 72, lanes])
            edges = [pltpu.roll(edges[-1], 1, 1)] + edges[:-1]
            for b in range(quads):
                q = p * quads + b
                lanes = pl.ds(q % 2 * LANES, LANES)
                real = grid_ref[q // 2, low_row : low_row + 32, lanes]
                imag = grid_ref[q // 2, low_row + 32 : low_row + 64, lanes]
                edge = edges[b]
                head_real = real[:8] + jnp.where(first, edge, 0.0)
                head_imag = imag[:8] + jnp.where(first, pltpu.roll(edge, held, 0), 0.0)
                real = jnp.concatenate([head_real, real[8:]], axis=0)
                imag = jnp.concatenate([head_imag, imag[8:]], axis=0)
                pieces.append(jnp.concatenate([real, imag], axis=1))
        high, low = split(jnp.concatenate(pieces, axis=0))
        spec_ref[k] = (
            jnp.dot(high, coarse_ref[0], preferred_element_type=jnp.float32)
            + jnp.dot(high, coarse_ref[1], preferred_element_type=jnp.float32)
            + jnp.dot(low, coarse_ref[0], preferred_element_type=jnp.float32)
        )

        def one_plane(p):
            inner = [[None] * pairs for r in range(4)]
            for t in range(pairs):
                column = []
                for b in range(quads):
                    row = pl.ds((p * quads + b) * 32 + t * 8, 8)
                    x = (spec_ref[k, row, :LANES], spec_ref[k, row, LANES:])
                    column.append(multiply(x, (twist_ref[0, b, t, 0], twist_ref[0, b, t, 1])))
                for r, z in enumerate(radix4(column)):
                    inner[r][t] = multiply(z, (twist_ref[1, r, t, 0], twist_ref[1, r, t, 1])) if r else z
            for r in range(4):
                for s, z in enumerate(radix4(inner[r])):
                    if s:
                        z = multiply(z, spin[s])
                    real = pltpu.roll(z[0], held, 0) + z[0] * flipper
                    imag = pltpu.roll(z[1], held, 0) + z[1] * flipper
                    at = r + 4 * s
                    term = real * screen_ref[p, at, 0] - imag * screen_ref[p, at, 1]
                    acc_ref[k, at] = acc_ref[k, at] + term if p else term

        for p in range(planes):
            one_plane(p)
        for at in range(16):
            img_refs[k][pl.ds(at, 8, stride=16), :] = acc_ref[k, at]

    span = per * 16

    def x_copies(k):
        copies = []
        for d in range(1, n_seat):
            for h in range(2):
                row = pl.multiple_of((held * h + seat_peer(d) * per) * 16, 16)
                copies.append(
                    pltpu.make_async_remote_copy(
                        src_ref=img_refs[k].at[pl.ds(row, span), :], dst_ref=xland_ref.at[k, d, h],
                        send_sem=x_send.at[k, d, h], recv_sem=x_recv.at[k, d, h],
                        device_id=(seat_peer(d) * CORES + core, bl), device_id_type=MESH,
                    )
                )
        return copies

    def b_copies(k):
        return [
            pltpu.make_async_remote_copy(
                src_ref=sum_ref.at[k, bl_peer(d)], dst_ref=bland_ref.at[k, d],
                send_sem=b_send.at[k, d], recv_sem=b_recv.at[k, d],
                device_id=(chan, bl_peer(d)), device_id_type=MESH,
            )
            for d in range(1, n_bl)
        ]

    share = per * NPIX // (n_bl * LANES)

    def gather_x(k, copies):
        for copy in copies:
            copy.wait()
        for h in range(2):
            row = pl.multiple_of((held * h + seat * per) * 16, 16)
            total = img_refs[k][pl.ds(row, span), :]
            for d in range(1, n_seat):
                total = total + xland_ref[k, d, h]
            for i in range(per):
                at = (i * 32 + h * 16) // share
                sum_ref[k, at : at + 16 // share] = total[i * 16 : (i + 1) * 16].reshape(16 // share, share, LANES)
        copies = b_copies(k)
        for copy in copies:
            copy.start()
        return copies

    x_flight = []
    b_flight = []
    for k in range(TAYLOR):
        transform(k)
        x_flight.append(x_copies(k))
        for copy in x_flight[-1]:
            copy.start()
    for k in range(TAYLOR):
        b_flight.append(gather_x(k, x_flight[k]))

    moments = msend_ref[...]
    for i, copy in enumerate(mom_copies):
        copy.wait()
        moments = moments + mland_ref[i]
    images = []
    for k in range(TAYLOR):
        total = sum_ref[k, bl]
        for d in range(1, n_bl):
            b_flight[k][d - 1].wait()
            total = total + bland_ref[k, d]
        images.append(total)
    solved = solve_taylor([moments[m : m + 1] for m in range(MOMENTS)], images)
    for k in range(TAYLOR):
        out_ref[k] = solved[k]


def strip_image(n_chan, n_bl, count, offsets, value, weight, kernel, tiles, plane, chans):
    consts = [jnp.asarray(t) for t in tables(n_chan)]
    tap_table, coarse, twist, screen = consts
    vmem = pl.BlockSpec(memory_space=pltpu.VMEM)
    hbm = pl.BlockSpec(memory_space=pl.ANY)
    slots = kernel.shape[1]
    n_seat = n_chan // CORES
    per = STRIP // n_chan
    share = per * NPIX // (n_bl * LANES)
    f32 = jnp.float32
    bf16 = jnp.bfloat16
    dma = pltpu.SemaphoreType.DMA
    block = [((rows_all, BLK), bf16), ((rows_all, BLK), bf16), ((BLK, LANES), bf16)]
    inputs = (count, offsets, value, weight, kernel, tiles, plane, chans)
    peers = n_seat * n_bl - 1
    scratch = [(x.shape, x.dtype) for x in inputs] + [
        (tap_table.shape[1:], bf16), (coarse.shape, bf16), (twist.shape, f32), (screen.shape[1:], f32),
        ((8, slots), f32), ((8, slots), f32), (kernel.shape, bf16),
        *block, *block,
        ((groups, rows_all, 2 * LANES), f32), ((8, BLK), f32), ((TAYLOR, planes * quads * 32, 2 * LANES), f32),
        ((TAYLOR, 16, 8, LANES), f32), ((LANES, LANES), f32), ((LANES, LANES), f32), ((LANES, LANES), f32),
        ((TAYLOR, n_seat, 2, per * 16, LANES), f32),
        ((TAYLOR, n_bl, share, LANES), f32), ((TAYLOR, n_bl, share, LANES), f32),
        ((8, LANES), f32), ((peers, 8, LANES), f32),
    ]
    return pl.pallas_call(
        functools.partial(strip_kernel, n_chan, n_bl),
        out_shape=pltpu.VMEM((TAYLOR, share, LANES), f32),
        in_specs=[hbm] * (len(inputs) + len(consts)),
        out_specs=vmem,
        scratch_shapes=[pltpu.VMEM(shape, kind) for shape, kind in scratch]
        + [
            dma((len(inputs) + len(consts),)), dma((2,)), dma((2,)),
            dma((TAYLOR, n_seat, 2)), dma((TAYLOR, n_seat, 2)), dma((peers,)), dma((peers,)),
            dma((TAYLOR, n_bl)), dma((TAYLOR, n_bl)),
        ],
        compiler_params=pltpu.CompilerParams(
            vmem_limit_bytes=56 * 1024 * 1024, collective_id=0, has_side_effects=True
        ),
        name="strip_image",
    )(*inputs, *consts)


def solution(mesh):
    n_chan = mesh.shape["chan"]
    n_bl = mesh.shape["bl"]

    def body(vis_value, vis_weight, kernel, tile_index, plane_index, chan_index, chan_offset, counts):
        out = strip_image(
            n_chan, n_bl, counts, chan_offset, vis_value[0, 0], vis_weight[0], kernel[0, 0],
            tile_index[0], plane_index[0], chan_index[0],
        )
        return out.reshape(TAYLOR, -1)

    in_specs = (
        P("chan", "bl", None, None),
        P("chan", "bl", None),
        P("chan", "bl", None, None),
        P("chan", "bl", None),
        P("chan", "bl", None),
        P("chan", "bl", None),
        P("chan", None),
        P("chan", "bl"),
    )
    out_specs = P(None, ("chan", "bl"))
    return jax.shard_map(body, mesh=mesh, in_specs=in_specs, out_specs=out_specs, check_vma=False)
```

```python
import functools

import numpy as np
import jax
import jax.numpy as jnp
from jax import lax
from jax.experimental import pallas as pl
from jax.experimental.pallas import tpu as pltpu
from jax.sharding import PartitionSpec as P

NPIX = 4096
TILE = 8
TAYLOR = 3
MOMENTS = 5
WPLANES = 8
STRIP = 8
LANES = 128
CORES = 2

two_pi = 2.0 * np.pi
w_step = 40.0
ntiles = NPIX // TILE
planes = WPLANES // 2
held = STRIP // CORES
quads = ntiles // LANES
groups = planes * quads // 2
pairs = TILE // 2
per_k = TILE * STRIP + 8
rows_all = TAYLOR * per_k
BLK = 512
low_scale = 256.0
f8 = jnp.float8_e4m3fn
MESH = pl.DeviceIdType.MESH


def split(x):
    high = x.astype(jnp.bfloat16)
    low = (x - high.astype(jnp.float32)).astype(jnp.bfloat16)
    return high, low


def cosine_series():
    g = 0.125 - 0.125 * np.cos(np.pi * (np.arange(64) + 0.5) / 64)
    fit = np.polynomial.Polynomial.fit(g, np.cos(two_pi * np.sqrt(g)), 8, domain=[0.0, 0.25])
    return [float(c) for c in fit.convert().coef]


cos_terms = cosine_series()


@functools.cache
def tables(n_chan):
    f32 = np.float32
    bf16 = jnp.bfloat16
    per = STRIP // n_chan

    def two(x):
        x = x.astype(f32)
        high = x.astype(bf16)
        return high, (x - high.astype(f32)).astype(bf16)

    slot = np.arange(held)
    strips = [(slot // per * CORES + core) * per + slot % per for core in range(CORES)]
    sub_e = np.arange(8) // held
    sub_l = np.arange(8) % held

    taps = np.zeros((CORES, 88, 2, TILE, TILE))
    for core in range(CORES):
        offset = strips[core] - STRIP // 2
        angle = two_pi * np.arange(TILE)[None, :] * offset[:, None] / NPIX
        for e in range(TILE + 1):
            for part, wave in enumerate((np.cos(angle), np.sin(angle))):
                if e < TILE:
                    rows = [part * 32 + e // 2 * 8 + e % 2 * held + slot]
                else:
                    rows = [64 + part * 8 + slot, 64 + part * 8 + held + slot]
                for row in rows:
                    if e < TILE:
                        taps[core, row, 0, :, e] = wave
                    if e > 0:
                        taps[core, row, 1, :, TILE - e] = wave
    taps[:, 80:] = 1.0
    tap_high, tap_low = two(taps.reshape(CORES, 88, 2 * TILE * TILE))
    tap_table = np.concatenate([tap_high, tap_low], axis=2)

    ids = np.arange(LANES)
    angle = two_pi * (ids[:, None] * ids[None, :] % LANES) / LANES
    cosine, sine = np.cos(angle), np.sin(angle)
    coarse = np.stack(two(np.block([[cosine, sine], [-sine, cosine]])))

    cell = (8 * np.arange(quads)[:, None, None] + 2 * np.arange(pairs)[None, :, None] + sub_e[None, None, :])[..., None]
    angle = two_pi * cell * ids / NPIX
    sign = 1.0 - 2.0 * ((cell + ids) % 2)
    twist = np.stack([np.cos(angle) * sign, np.sin(angle) * sign], axis=2)
    e = 2 * np.arange(pairs)[None, :, None] + sub_e[None, None, :]
    angle = np.broadcast_to(two_pi * (np.arange(4)[:, None, None] * e)[..., None] / 32, (4, pairs, 8, LANES))
    inner = np.stack([np.cos(angle), np.sin(angle)], axis=2)
    twist = np.stack([twist, inner]).astype(f32)

    cell_size = 0.5 / NPIX
    screens = []
    for core in range(CORES):
        x = (strips[core][sub_l] - STRIP // 2) * cell_size
        column = ids[None, None, :] + LANES * (np.arange(16)[:, None, None] + 16 * sub_e[None, :, None])
        y = (column - NPIX // 2) * cell_size
        radius = x[None, :, None] ** 2 + y**2
        lowered = -radius / (1.0 + np.sqrt(1.0 - radius))
        w = w_step * (np.arange(planes) - 0.5 * (WPLANES - 1))
        angle = two_pi * w[:, None, None, None] * lowered[None]
        screens.append(np.stack([np.cos(angle), np.sin(angle)], axis=2))
    screen = np.stack(screens).astype(f32)
    return tap_table, coarse, twist, screen


def solve_taylor(moments, images):
    entry_00, entry_01, entry_02 = (moments[0], moments[1], moments[2])
    entry_11, entry_12, entry_22 = (moments[2], moments[3], moments[4])
    minor_00 = entry_11 * entry_22 - entry_12 * entry_12
    minor_01 = entry_02 * entry_12 - entry_01 * entry_22
    minor_02 = entry_01 * entry_12 - entry_02 * entry_11
    minor_11 = entry_00 * entry_22 - entry_02 * entry_02
    minor_12 = entry_01 * entry_02 - entry_00 * entry_12
    minor_22 = entry_00 * entry_11 - entry_01 * entry_01
    determinant = entry_00 * minor_00 + entry_01 * minor_01 + entry_02 * minor_02
    first = (minor_00 * images[0] + minor_01 * images[1] + minor_02 * images[2]) / determinant
    second = (minor_01 * images[0] + minor_11 * images[1] + minor_12 * images[2]) / determinant
    third = (minor_02 * images[0] + minor_12 * images[1] + minor_22 * images[2]) / determinant
    return first, second, third


def multiply(a, b):
    return a[0] * b[0] - a[1] * b[1], a[0] * b[1] + a[1] * b[0]


def radix4(x):
    a = (x[0][0] + x[2][0], x[0][1] + x[2][1])
    b = (x[0][0] - x[2][0], x[0][1] - x[2][1])
    c = (x[1][0] + x[3][0], x[1][1] + x[3][1])
    d = (x[1][0] - x[3][0], x[1][1] - x[3][1])
    return (
        (a[0] + c[0], a[1] + c[1]), (b[0] - d[1], b[1] + d[0]),
        (a[0] - c[0], a[1] - c[1]), (b[0] + d[1], b[1] - d[0]),
    )


def strip_kernel(
    n_chan, n_bl, count_hbm, offset_hbm, value_hbm, weight_hbm, kernel_hbm, tile_hbm, plane_hbm, chan_hbm,
    tap_hbm, coarse_hbm, twist_hbm, screen_hbm, out_ref,
    count_ref, offset_ref, value_ref, weight_ref, kernel_ref, tile_ref, plane_ref, chan_ref,
    tap_ref, coarse_ref, twist_ref, screen_ref, meta_ref, meta_land, taps_land,
    high0_ref, low0_ref, code0_ref, high1_ref, low1_ref, code1_ref,
    grid_ref, mom_ref, spec_ref, acc_ref, img0_ref, img1_ref, img2_ref,
    xland_ref, sum_ref, bland_ref, msend_ref, mxland_ref, msum_ref, mland_ref,
    load_sem, pair_send, pair_recv, x_send, x_recv, xm_send, xm_recv, b_send, b_recv, bm_send, bm_recv,
):
    chan = lax.axis_index("chan")
    bl = lax.axis_index("bl")
    core = lax.rem(chan, CORES)
    seat = chan // CORES
    n_seat = n_chan // CORES
    per = STRIP // n_chan
    img_refs = (img0_ref, img1_ref, img2_ref)
    slots = kernel_ref.shape[1]

    def seat_peer(d):
        return lax.rem(seat + d, n_seat)

    def bl_peer(d):
        return lax.rem(bl + d, n_bl)

    mate = (chan + 1 - 2 * core, bl)
    loads = [
        pltpu.make_async_copy(source, target, load_sem.at[i])
        for i, (source, target) in enumerate((
            (count_hbm, count_ref), (offset_hbm, offset_ref), (value_hbm, value_ref), (weight_hbm, weight_ref),
            (tile_hbm, tile_ref), (plane_hbm, plane_ref), (chan_hbm, chan_ref),
            (kernel_hbm, kernel_ref), (tap_hbm.at[core], tap_ref), (coarse_hbm, coarse_ref),
            (twist_hbm, twist_ref), (screen_hbm.at[core], screen_ref),
        ))
    ]
    for load in loads:
        load.start()

    barrier = pltpu.get_barrier_semaphore()
    pl.semaphore_signal(barrier, inc=1, device_id=mate, device_id_type=MESH)
    for d in range(1, n_seat):
        pl.semaphore_signal(barrier, inc=1, device_id=(seat_peer(d) * CORES + core, bl), device_id_type=MESH)
    for d in range(1, n_bl):
        pl.semaphore_signal(barrier, inc=1, device_id=(chan, bl_peer(d)), device_id_type=MESH)

    mom_ref[...] = jnp.zeros_like(mom_ref)
    for load in loads[:7]:
        load.wait()

    slot = lax.broadcasted_iota(jnp.int32, (1, slots), 1)
    tiles = tile_ref[...]
    plane = plane_ref[...]
    chans = chan_ref[...]
    coord = jnp.zeros((1, slots), jnp.float32)
    for c in range(offset_ref.shape[1]):
        coord = jnp.where(chans == c, offset_ref[0:1, c : c + 1], coord)
    weight = jnp.where(slot < count_ref[...], weight_ref[...].astype(jnp.float32), 0.0)
    value = value_ref[...].astype(jnp.float32)
    flip = plane >= planes
    v_tile = tiles & (ntiles - 1)
    v_tile = jnp.where(flip, ntiles - 1 - v_tile, v_tile)
    fold = jnp.where(flip, WPLANES - 1 - plane, plane)
    place = (fold * quads + (v_tile & (quads - 1))) * LANES + lax.shift_right_logical(v_tile, quads.bit_length() - 1)
    meta_ref[0:1, :] = weight * value[0:1]
    meta_ref[1:2, :] = weight * value[1:2]
    meta_ref[2:3, :] = coord
    meta_ref[3:4, :] = weight
    meta_ref[4:5, :] = (lax.shift_right_logical(tiles, ntiles.bit_length() - 1) - ntiles // 2).astype(jnp.float32)
    meta_ref[5:6, :] = place.astype(jnp.float32)
    meta_ref[6:7, :] = jnp.where(flip, -1.0, 1.0)
    meta_ref[7:8, :] = jnp.zeros((1, slots), jnp.float32)

    sub = lax.broadcasted_iota(jnp.int32, (8, 1), 0)
    first = sub < held
    local = lax.rem(sub, held)
    strip = (local // per * CORES + core) * per + lax.rem(local, per) - STRIP // 2
    turn = strip.astype(jnp.float32) * (1.0 / ntiles)
    quarter = jnp.where(first, 0.0, 0.25)

    for load in loads[7:9]:
        load.wait()

    buffers = ((high0_ref, low0_ref, code0_ref), (high1_ref, low1_ref, code1_ref))

    def prepare(taps_ref, rows_ref, block, buffer):
        high_ref, low_ref, code_ref = buffer
        here = pl.ds(block * BLK, BLK)
        base_real = rows_ref[0:1, here]
        base_imag = rows_ref[1:2, here]
        coord = rows_ref[2:3, here]
        weight = rows_ref[3:4, here]
        u_off = rows_ref[4:5, here]
        place = rows_ref[5:6, here]
        sign = rows_ref[6:7, here]
        taps = taps_ref[:, here]
        plain = taps * jnp.maximum(sign, 0.0).astype(jnp.bfloat16)
        turned = taps * jnp.maximum(-sign, 0.0).astype(jnp.bfloat16)
        sums = jnp.dot(
            tap_ref[...], jnp.concatenate([plain, turned, plain, turned], axis=0),
            preferred_element_type=jnp.float32,
        )
        cycle = u_off * turn - quarter
        cycle = cycle - jnp.floor(cycle + 0.5)
        square = cycle * cycle
        wave = jnp.full_like(square, cos_terms[-1])
        for term in cos_terms[-2::-1]:
            wave = wave * square + term
        other = pltpu.roll(wave, held, 0)
        cosine = jnp.where(first, wave, other)
        sine = jnp.where(first, other, wave)
        z_real = base_real * cosine - base_imag * sine
        z_imag = base_real * sine + base_imag * cosine
        s_real = z_real * sign
        s_imag = z_imag * sign
        sum_real = sums[0:32].reshape(pairs, 8, BLK)
        sum_imag = sums[32:64].reshape(pairs, 8, BLK)
        part_real = (sum_real * z_real[None] - sum_imag * z_imag[None]).reshape(32, BLK)
        part_imag = (sum_real * s_imag[None] + sum_imag * s_real[None]).reshape(32, BLK)
        edge = sums[64:72] * jnp.where(first, z_real, s_imag) + sums[72:80] * jnp.where(first, -z_imag, s_real)
        part = jnp.concatenate([part_real, part_imag, edge], axis=0)
        parts = [part]
        for k in range(1, TAYLOR):
            parts.append(parts[-1] * coord)
        parts = jnp.concatenate(parts, axis=0)
        high = parts.astype(jnp.bfloat16)
        high_ref[...] = high
        low_ref[...] = ((parts - high.astype(jnp.float32)) * low_scale).astype(f8)

        weighted = weight * sums[80:81]
        power = weighted
        for m in range(MOMENTS):
            mom_ref[m : m + 1, :] += power
            power = power * coord

        lane = lax.broadcasted_iota(jnp.int32, (BLK, LANES), 1).astype(jnp.float32)
        column = jnp.transpose(jnp.broadcast_to(place, (LANES, BLK)))
        level = (column - lane) * (1.0 / LANES)
        code = jnp.where(jnp.floor(level) == level, level, -1.0).astype(jnp.bfloat16)
        one = jnp.bfloat16(1.0)
        zero = jnp.bfloat16(0.0)
        for q in range(planes * quads):
            code_ref[:, q * LANES : (q + 1) * LANES] = jnp.where(code == jnp.bfloat16(q), one, zero).astype(f8)

    def scatter(buffer, fresh):
        high_ref, low_ref, code_ref = buffer
        for g in range(groups):
            hot = code_ref[:, g * 2 * LANES : (g + 1) * 2 * LANES]
            rest = jnp.dot(low_ref[...], hot, preferred_element_type=jnp.float32)
            update = jnp.dot(high_ref[...], hot, preferred_element_type=jnp.float32) + rest * (1.0 / low_scale)
            if fresh:
                grid_ref[g] = update
            else:
                grid_ref[g] += update

    blocks = slots // BLK
    swaps = [
        pltpu.make_async_remote_copy(
            src_ref=source, dst_ref=target, send_sem=pair_send.at[i], recv_sem=pair_recv.at[i],
            device_id=mate, device_id_type=MESH,
        )
        for i, (source, target) in enumerate(((kernel_ref, taps_land), (meta_ref, meta_land)))
    ]
    order = [(kernel_ref, meta_ref, j) for j in range(blocks)] + [(taps_land, meta_land, j) for j in range(blocks)]
    prepare(*order[0], buffers[0])
    for j in range(2 * blocks):
        if j == 1:
            pl.semaphore_wait(barrier, 1 + n_seat - 1 + n_bl - 1)
            for swap in swaps:
                swap.start()
        if j + 1 == blocks:
            for swap in swaps:
                swap.wait()
        if j + 1 < 2 * blocks:
            prepare(*order[j + 1], buffers[(j + 1) % 2])
        scatter(buffers[j % 2], j == 0)

    msend_ref[...] = jnp.broadcast_to(jnp.sum(mom_ref[...], axis=1, keepdims=True), msend_ref.shape)
    def drain(ref, send, recv):
        pltpu.make_async_copy(ref, ref, send).wait()
        pltpu.make_async_copy(ref, ref, recv).wait()

    for d in range(1, n_seat):
        pltpu.make_async_remote_copy(
            src_ref=msend_ref, dst_ref=mxland_ref.at[d - 1], send_sem=xm_send, recv_sem=xm_recv,
            device_id=(seat_peer(d) * CORES + core, bl), device_id_type=MESH,
        ).start()

    for load in loads[9:]:
        load.wait()
    flipper = jnp.where(first, 1.0, -1.0)
    spin = [
        (jnp.where(first, 1.0, float(np.cos(two_pi * s / 8))), jnp.where(first, 0.0, float(np.sin(two_pi * s / 8))))
        for s in range(4)
    ]

    def transform(k):
        low_row = k * per_k
        pieces = []
        for p in range(planes):
            edges = []
            for b in range(quads):
                q = p * quads + b
                lanes = pl.ds(q % 2 * LANES, LANES)
                edges.append(grid_ref[q // 2, low_row + 64 : low_row + 72, lanes])
            edges = [pltpu.roll(edges[-1], 1, 1)] + edges[:-1]
            for b in range(quads):
                q = p * quads + b
                lanes = pl.ds(q % 2 * LANES, LANES)
                real = grid_ref[q // 2, low_row : low_row + 32, lanes]
                imag = grid_ref[q // 2, low_row + 32 : low_row + 64, lanes]
                edge = edges[b]
                head_real = real[:8] + jnp.where(first, edge, 0.0)
                head_imag = imag[:8] + jnp.where(first, pltpu.roll(edge, held, 0), 0.0)
                real = jnp.concatenate([head_real, real[8:]], axis=0)
                imag = jnp.concatenate([head_imag, imag[8:]], axis=0)
                pieces.append(jnp.concatenate([real, imag], axis=1))
        high, low = split(jnp.concatenate(pieces, axis=0))
        spec_ref[k] = (
            jnp.dot(high, coarse_ref[0], preferred_element_type=jnp.float32)
            + jnp.dot(high, coarse_ref[1], preferred_element_type=jnp.float32)
            + jnp.dot(low, coarse_ref[0], preferred_element_type=jnp.float32)
        )

        def one_plane(p):
            inner = [[None] * pairs for r in range(4)]
            for t in range(pairs):
                column = []
                for b in range(quads):
                    row = pl.ds((p * quads + b) * 32 + t * 8, 8)
                    x = (spec_ref[k, row, :LANES], spec_ref[k, row, LANES:])
                    column.append(multiply(x, (twist_ref[0, b, t, 0], twist_ref[0, b, t, 1])))
                for r, z in enumerate(radix4(column)):
                    inner[r][t] = multiply(z, (twist_ref[1, r, t, 0], twist_ref[1, r, t, 1])) if r else z
            for r in range(4):
                for s, z in enumerate(radix4(inner[r])):
                    if s:
                        z = multiply(z, spin[s])
                    real = pltpu.roll(z[0], held, 0) + z[0] * flipper
                    imag = pltpu.roll(z[1], held, 0) + z[1] * flipper
                    at = r + 4 * s
                    term = real * screen_ref[p, at, 0] - imag * screen_ref[p, at, 1]
                    acc_ref[k, at] = acc_ref[k, at] + term if p else term

        for p in range(planes):
            one_plane(p)
        for at in range(16):
            img_refs[k][pl.ds(at, 8, stride=16), :] = acc_ref[k, at]

    span = per * 16

    def send_x(k):
        for d in range(1, n_seat):
            for h in range(2):
                row = pl.multiple_of((held * h + seat_peer(d) * per) * 16, 16)
                pltpu.make_async_remote_copy(
                    src_ref=img_refs[k].at[pl.ds(row, span), :], dst_ref=xland_ref.at[k, d - 1, h],
                    send_sem=x_send.at[k], recv_sem=x_recv.at[k],
                    device_id=(seat_peer(d) * CORES + core, bl), device_id_type=MESH,
                ).start()

    def send_b(k):
        for d in range(1, n_bl):
            pltpu.make_async_remote_copy(
                src_ref=sum_ref.at[k, bl_peer(d)], dst_ref=bland_ref.at[k, d - 1],
                send_sem=b_send.at[k], recv_sem=b_recv.at[k],
                device_id=(chan, bl_peer(d)), device_id_type=MESH,
            ).start()

    share = per * NPIX // (n_bl * LANES)

    def gather_x(k):
        drain(xland_ref.at[k], x_send.at[k], x_recv.at[k])
        for h in range(2):
            row = pl.multiple_of((held * h + seat * per) * 16, 16)
            total = img_refs[k][pl.ds(row, span), :]
            for d in range(1, n_seat):
                total = total + xland_ref[k, d - 1, h]
            for i in range(per):
                at = (i * 32 + h * 16) // share
                sum_ref[k, at : at + 16 // share] = total[i * 16 : (i + 1) * 16].reshape(16 // share, share, LANES)
        send_b(k)

    for k in range(TAYLOR):
        transform(k)
        send_x(k)
    drain(mxland_ref, xm_send, xm_recv)
    total = msend_ref[...]
    for d in range(1, n_seat):
        total = total + mxland_ref[d - 1]
    msum_ref[...] = total
    for d in range(1, n_bl):
        pltpu.make_async_remote_copy(
            src_ref=msum_ref, dst_ref=mland_ref.at[d - 1], send_sem=bm_send, recv_sem=bm_recv,
            device_id=(chan, bl_peer(d)), device_id_type=MESH,
        ).start()
    for k in range(TAYLOR):
        gather_x(k)

    drain(mland_ref, bm_send, bm_recv)
    moments = msum_ref[...]
    for d in range(1, n_bl):
        moments = moments + mland_ref[d - 1]
    images = []
    for k in range(TAYLOR):
        drain(bland_ref.at[k], b_send.at[k], b_recv.at[k])
        total = sum_ref[k, bl]
        for d in range(1, n_bl):
            total = total + bland_ref[k, d - 1]
        images.append(total)
    solved = solve_taylor([moments[m : m + 1] for m in range(MOMENTS)], images)
    for k in range(TAYLOR):
        out_ref[k] = solved[k]


def strip_image(n_chan, n_bl, count, offsets, value, weight, kernel, tiles, plane, chans):
    consts = [jnp.asarray(t) for t in tables(n_chan)]
    tap_table, coarse, twist, screen = consts
    vmem = pl.BlockSpec(memory_space=pltpu.VMEM)
    hbm = pl.BlockSpec(memory_space=pl.ANY)
    slots = kernel.shape[1]
    n_seat = n_chan // CORES
    per = STRIP // n_chan
    share = per * NPIX // (n_bl * LANES)
    f32 = jnp.float32
    bf16 = jnp.bfloat16
    dma = pltpu.SemaphoreType.DMA
    block = [((rows_all, BLK), bf16), ((rows_all, BLK), f8), ((BLK, planes * ntiles), f8)]
    inputs = (count, offsets, value, weight, kernel, tiles, plane, chans)
    scratch = [(x.shape, x.dtype) for x in inputs] + [
        (tap_table.shape[1:], bf16), (coarse.shape, bf16), (twist.shape, f32), (screen.shape[1:], f32),
        ((8, slots), f32), ((8, slots), f32), (kernel.shape, bf16),
        *block, *block,
        ((groups, rows_all, 2 * LANES), f32), ((8, BLK), f32), ((TAYLOR, planes * quads * 32, 2 * LANES), f32),
        ((TAYLOR, 16, 8, LANES), f32), ((LANES, LANES), f32), ((LANES, LANES), f32), ((LANES, LANES), f32),
        ((TAYLOR, n_seat - 1, 2, per * 16, LANES), f32),
        ((TAYLOR, n_bl, share, LANES), f32), ((TAYLOR, n_bl - 1, share, LANES), f32),
        ((8, LANES), f32), ((n_seat - 1, 8, LANES), f32), ((8, LANES), f32), ((n_bl - 1, 8, LANES), f32),
    ]
    return pl.pallas_call(
        functools.partial(strip_kernel, n_chan, n_bl),
        out_shape=pltpu.VMEM((TAYLOR, share, LANES), f32),
        in_specs=[hbm] * (len(inputs) + len(consts)),
        out_specs=vmem,
        scratch_shapes=[pltpu.VMEM(shape, kind) for shape, kind in scratch]
        + [
            dma((len(inputs) + len(consts),)), dma((2,)), dma((2,)),
            dma((TAYLOR,)), dma((TAYLOR,)), dma, dma, dma((TAYLOR,)), dma((TAYLOR,)), dma, dma,
        ],
        compiler_params=pltpu.CompilerParams(
            vmem_limit_bytes=56 * 1024 * 1024, collective_id=0, has_side_effects=True
        ),
        name="strip_image",
    )(*inputs, *consts)


def solution(mesh):
    n_chan = mesh.shape["chan"]
    n_bl = mesh.shape["bl"]

    def body(vis_value, vis_weight, kernel, tile_index, plane_index, chan_index, chan_offset, counts):
        out = strip_image(
            n_chan, n_bl, counts, chan_offset, vis_value[0, 0], vis_weight[0], kernel[0, 0],
            tile_index[0], plane_index[0], chan_index[0],
        )
        return out.reshape(TAYLOR, -1)

    in_specs = (
        P("chan", "bl", None, None),
        P("chan", "bl", None),
        P("chan", "bl", None, None),
        P("chan", "bl", None),
        P("chan", "bl", None),
        P("chan", "bl", None),
        P("chan", None),
        P("chan", "bl"),
    )
    out_specs = P(None, ("chan", "bl"))
    return jax.shard_map(body, mesh=mesh, in_specs=in_specs, out_specs=out_specs, check_vma=False)
```

```python
import functools

import numpy as np
import jax
import jax.numpy as jnp
from jax import lax
from jax.experimental import pallas as pl
from jax.experimental.pallas import tpu as pltpu
from jax.sharding import PartitionSpec as P

NPIX = 4096
TILE = 8
TAYLOR = 3
MOMENTS = 5
WPLANES = 8
STRIP = 8
LANES = 128
CORES = 2

two_pi = 2.0 * np.pi
w_step = 40.0
ntiles = NPIX // TILE
planes = WPLANES // 2
held = STRIP // CORES
quads = ntiles // LANES
groups = planes * quads // 2
pairs = TILE // 2
per_k = TILE * STRIP + 8
rows_all = TAYLOR * per_k
BLK = 512
low_scale = 256.0
f8 = jnp.float8_e4m3fn
MESH = pl.DeviceIdType.MESH


def split(x):
    high = x.astype(jnp.bfloat16)
    low = (x - high.astype(jnp.float32)).astype(jnp.bfloat16)
    return high, low


def cosine_series():
    g = 0.125 - 0.125 * np.cos(np.pi * (np.arange(64) + 0.5) / 64)
    fit = np.polynomial.Polynomial.fit(g, np.cos(two_pi * np.sqrt(g)), 8, domain=[0.0, 0.25])
    return [float(c) for c in fit.convert().coef]


cos_terms = cosine_series()


@functools.cache
def tables(n_chan):
    f32 = np.float32
    bf16 = jnp.bfloat16
    per = STRIP // n_chan

    def two(x):
        x = x.astype(f32)
        high = x.astype(bf16)
        return high, (x - high.astype(f32)).astype(bf16)

    slot = np.arange(held)
    strips = [(slot // per * CORES + core) * per + slot % per for core in range(CORES)]
    sub_e = np.arange(8) // held
    sub_l = np.arange(8) % held

    taps = np.zeros((CORES, 88, 2, TILE, TILE))
    for core in range(CORES):
        offset = strips[core] - STRIP // 2
        angle = two_pi * np.arange(TILE)[None, :] * offset[:, None] / NPIX
        for e in range(TILE + 1):
            for part, wave in enumerate((np.cos(angle), np.sin(angle))):
                if e < TILE:
                    rows = [part * 32 + e // 2 * 8 + e % 2 * held + slot]
                else:
                    rows = [64 + part * 8 + slot, 64 + part * 8 + held + slot]
                for row in rows:
                    if e < TILE:
                        taps[core, row, 0, :, e] = wave
                    if e > 0:
                        taps[core, row, 1, :, TILE - e] = wave
    taps[:, 80:] = 1.0
    tap_high, tap_low = two(taps.reshape(CORES, 88, 2 * TILE * TILE))
    tap_table = np.concatenate([tap_high, tap_low], axis=2)

    ids = np.arange(LANES)
    angle = two_pi * (ids[:, None] * ids[None, :] % LANES) / LANES
    coarse = []
    for b in range(quads):
        angle = two_pi * (ids[:, None] * ids[None, :] % LANES) / LANES + two_pi * 8 * b * ids[None, :] / NPIX
        cosine, sine = np.cos(angle), np.sin(angle)
        coarse.append(np.stack(two(np.block([[cosine, sine], [-sine, cosine]]))))
    coarse = np.stack(coarse)

    e = (2 * np.arange(pairs)[:, None] + sub_e[None, :])[..., None]
    column = ids + LANES * np.arange(4)[:, None, None, None]
    sign = 1.0 - 2.0 * ((e + column) % 2)
    angle = two_pi * e * column / NPIX
    twist = np.stack([np.cos(angle) * sign, np.sin(angle) * sign], axis=2).astype(f32)

    cell_size = 0.5 / NPIX
    screens = []
    for core in range(CORES):
        x = (strips[core][sub_l] - STRIP // 2) * cell_size
        column = ids[None, None, :] + LANES * (np.arange(16)[:, None, None] + 16 * sub_e[None, :, None])
        y = (column - NPIX // 2) * cell_size
        radius = x[None, :, None] ** 2 + y**2
        lowered = -radius / (1.0 + np.sqrt(1.0 - radius))
        w = w_step * (np.arange(planes) - 0.5 * (WPLANES - 1))
        angle = two_pi * w[:, None, None, None] * lowered[None]
        screens.append(np.stack([np.cos(angle), np.sin(angle)], axis=2))
    screen = np.stack(screens).astype(f32)
    return tap_table, coarse, twist, screen


def solve_taylor(moments, images):
    entry_00, entry_01, entry_02 = (moments[0], moments[1], moments[2])
    entry_11, entry_12, entry_22 = (moments[2], moments[3], moments[4])
    minor_00 = entry_11 * entry_22 - entry_12 * entry_12
    minor_01 = entry_02 * entry_12 - entry_01 * entry_22
    minor_02 = entry_01 * entry_12 - entry_02 * entry_11
    minor_11 = entry_00 * entry_22 - entry_02 * entry_02
    minor_12 = entry_01 * entry_02 - entry_00 * entry_12
    minor_22 = entry_00 * entry_11 - entry_01 * entry_01
    determinant = entry_00 * minor_00 + entry_01 * minor_01 + entry_02 * minor_02
    first = (minor_00 * images[0] + minor_01 * images[1] + minor_02 * images[2]) / determinant
    second = (minor_01 * images[0] + minor_11 * images[1] + minor_12 * images[2]) / determinant
    third = (minor_02 * images[0] + minor_12 * images[1] + minor_22 * images[2]) / determinant
    return first, second, third


def multiply(a, b):
    return a[0] * b[0] - a[1] * b[1], a[0] * b[1] + a[1] * b[0]


def radix4(x):
    a = (x[0][0] + x[2][0], x[0][1] + x[2][1])
    b = (x[0][0] - x[2][0], x[0][1] - x[2][1])
    c = (x[1][0] + x[3][0], x[1][1] + x[3][1])
    d = (x[1][0] - x[3][0], x[1][1] - x[3][1])
    return (
        (a[0] + c[0], a[1] + c[1]), (b[0] - d[1], b[1] + d[0]),
        (a[0] - c[0], a[1] - c[1]), (b[0] + d[1], b[1] - d[0]),
    )


def strip_kernel(
    n_chan, n_bl, count_hbm, offset_hbm, value_hbm, weight_hbm, kernel_hbm, tile_hbm, plane_hbm, chan_hbm,
    tap_hbm, coarse_hbm, twist_hbm, screen_hbm, out_ref,
    count_ref, offset_ref, value_ref, weight_ref, kernel_ref, tile_ref, plane_ref, chan_ref,
    tap_ref, coarse_ref, twist_ref, screen_ref, meta_ref, meta_land, taps_land,
    high0_ref, low0_ref, code0_ref, high1_ref, low1_ref, code1_ref,
    grid0_ref, grid1_ref, grid2_ref, mom_ref, spec_ref, acc_ref, img0_ref, img1_ref, img2_ref,
    xland_ref, sum_ref, bland_ref, msend_ref, mxland_ref, msum_ref, mland_ref,
    load_sem, pair_send, pair_recv, x_send, x_recv, xm_send, xm_recv, b_send, b_recv, bm_send, bm_recv,
):
    chan = lax.axis_index("chan")
    bl = lax.axis_index("bl")
    core = lax.rem(chan, CORES)
    seat = chan // CORES
    n_seat = n_chan // CORES
    per = STRIP // n_chan
    img_refs = (img0_ref, img1_ref, img2_ref)
    slots = kernel_ref.shape[1]

    def seat_peer(d):
        return lax.rem(seat + d, n_seat)

    def bl_peer(d):
        return lax.rem(bl + d, n_bl)

    mate = (chan + 1 - 2 * core, bl)
    loads = [
        pltpu.make_async_copy(source, target, load_sem.at[i])
        for i, (source, target) in enumerate((
            (count_hbm, count_ref), (offset_hbm, offset_ref), (value_hbm, value_ref), (weight_hbm, weight_ref),
            (tile_hbm, tile_ref), (plane_hbm, plane_ref), (chan_hbm, chan_ref),
            (kernel_hbm, kernel_ref), (tap_hbm.at[core], tap_ref), (coarse_hbm, coarse_ref),
            (twist_hbm, twist_ref), (screen_hbm.at[core], screen_ref),
        ))
    ]
    for load in loads[7:9] + loads[:7] + loads[9:]:
        load.start()

    barrier = pltpu.get_barrier_semaphore()
    pl.semaphore_signal(barrier, inc=1, device_id=mate, device_id_type=MESH)
    for d in range(1, n_seat):
        pl.semaphore_signal(barrier, inc=1, device_id=(seat_peer(d) * CORES + core, bl), device_id_type=MESH)
    for d in range(1, n_bl):
        pl.semaphore_signal(barrier, inc=1, device_id=(chan, bl_peer(d)), device_id_type=MESH)

    mom_ref[...] = jnp.zeros_like(mom_ref)
    for load in loads[:7]:
        load.wait()

    slot = lax.broadcasted_iota(jnp.int32, (1, slots), 1)
    tiles = tile_ref[...]
    plane = plane_ref[...]
    chans = chan_ref[...]
    coord = jnp.zeros((1, slots), jnp.float32)
    for c in range(offset_ref.shape[1]):
        coord = jnp.where(chans == c, offset_ref[0:1, c : c + 1], coord)
    weight = jnp.where(slot < count_ref[...], weight_ref[...].astype(jnp.float32), 0.0)
    value = value_ref[...].astype(jnp.float32)
    flip = plane >= planes
    v_tile = tiles & (ntiles - 1)
    v_tile = jnp.where(flip, ntiles - 1 - v_tile, v_tile)
    fold = jnp.where(flip, WPLANES - 1 - plane, plane)
    place = (fold * quads + (v_tile & (quads - 1))) * LANES + lax.shift_right_logical(v_tile, quads.bit_length() - 1)
    meta_ref[0:1, :] = weight * value[0:1]
    meta_ref[1:2, :] = weight * value[1:2]
    meta_ref[2:3, :] = coord
    meta_ref[3:4, :] = weight
    meta_ref[4:5, :] = (lax.shift_right_logical(tiles, ntiles.bit_length() - 1) - ntiles // 2).astype(jnp.float32)
    meta_ref[5:6, :] = place.astype(jnp.float32)
    meta_ref[6:7, :] = jnp.where(flip, -1.0, 1.0)
    meta_ref[7:8, :] = jnp.zeros((1, slots), jnp.float32)

    sub = lax.broadcasted_iota(jnp.int32, (8, 1), 0)
    first = sub < held
    local = lax.rem(sub, held)
    strip = (local // per * CORES + core) * per + lax.rem(local, per) - STRIP // 2
    turn = strip.astype(jnp.float32) * (1.0 / ntiles)
    quarter = jnp.where(first, 0.0, 0.25)

    for load in loads[7:9]:
        load.wait()

    buffers = ((high0_ref, low0_ref, code0_ref), (high1_ref, low1_ref, code1_ref))

    def prepare(taps_ref, rows_ref, block, buffer):
        high_ref, low_ref, code_ref = buffer
        start, size = block
        here = pl.ds(start, size)
        base_real = rows_ref[0:1, here]
        base_imag = rows_ref[1:2, here]
        coord = rows_ref[2:3, here]
        weight = rows_ref[3:4, here]
        u_off = rows_ref[4:5, here]
        place = rows_ref[5:6, here]
        sign = rows_ref[6:7, here]
        taps = taps_ref[:, here]
        plain = taps * jnp.maximum(sign, 0.0).astype(jnp.bfloat16)
        turned = taps * jnp.maximum(-sign, 0.0).astype(jnp.bfloat16)
        sums = jnp.dot(
            tap_ref[...], jnp.concatenate([plain, turned, plain, turned], axis=0),
            preferred_element_type=jnp.float32,
        )
        cycle = u_off * turn - quarter
        cycle = cycle - jnp.floor(cycle + 0.5)
        square = cycle * cycle
        wave = jnp.full_like(square, cos_terms[-1])
        for term in cos_terms[-2::-1]:
            wave = wave * square + term
        other = pltpu.roll(wave, held, 0)
        cosine = jnp.where(first, wave, other)
        sine = jnp.where(first, other, wave)
        z_real = base_real * cosine - base_imag * sine
        z_imag = base_real * sine + base_imag * cosine
        s_real = z_real * sign
        s_imag = z_imag * sign
        sum_real = sums[0:32].reshape(pairs, 8, size)
        sum_imag = sums[32:64].reshape(pairs, 8, size)
        part_real = (sum_real * z_real[None] - sum_imag * z_imag[None]).reshape(32, size)
        part_imag = (sum_real * s_imag[None] + sum_imag * s_real[None]).reshape(32, size)
        edge = sums[64:72] * jnp.where(first, z_real, s_imag) + sums[72:80] * jnp.where(first, -z_imag, s_real)
        part = jnp.concatenate([part_real, part_imag, edge], axis=0)
        parts = [part]
        for k in range(1, TAYLOR):
            parts.append(parts[-1] * coord)
        parts = jnp.concatenate(parts, axis=0)
        high = parts.astype(jnp.bfloat16)
        high_ref[:, :size] = high
        low_ref[:, :size] = ((parts - high.astype(jnp.float32)) * low_scale).astype(f8)

        weighted = weight * sums[80:81]
        power = weighted
        for m in range(MOMENTS):
            mom_ref[m : m + 1, :size] += power
            power = power * coord

        lane = lax.broadcasted_iota(jnp.int32, (size, LANES), 1).astype(jnp.float32)
        column = jnp.transpose(jnp.broadcast_to(place, (LANES, size)))
        level = (column - lane) * (1.0 / LANES)
        code = jnp.where(jnp.floor(level) == level, level, -1.0).astype(jnp.bfloat16)
        one = jnp.bfloat16(1.0)
        zero = jnp.bfloat16(0.0)
        for q in range(planes * quads):
            code_ref[:size, q * LANES : (q + 1) * LANES] = jnp.where(code == jnp.bfloat16(q), one, zero).astype(f8)

    grid_refs = (grid0_ref, grid1_ref, grid2_ref)

    def scatter(buffer, size, fresh, ks=tuple(range(TAYLOR))):
        high_ref, low_ref, code_ref = buffer
        these = pl.ds(ks[0] * per_k, len(ks) * per_k)
        for g in range(groups):
            hot = code_ref[:size, g * 2 * LANES : (g + 1) * 2 * LANES]
            rest = jnp.dot(low_ref[these, :size], hot, preferred_element_type=jnp.float32)
            update = jnp.dot(high_ref[these, :size], hot, preferred_element_type=jnp.float32) + rest * (1.0 / low_scale)
            for i, k in enumerate(ks):
                piece = update[i * per_k : (i + 1) * per_k]
                if fresh:
                    grid_refs[k][g] = piece
                else:
                    grid_refs[k][g] += piece

    swaps = [
        pltpu.make_async_remote_copy(
            src_ref=source, dst_ref=target, send_sem=pair_send.at[i], recv_sem=pair_recv.at[i],
            device_id=mate, device_id_type=MESH,
        )
        for i, (source, target) in enumerate(((kernel_ref, taps_land), (meta_ref, meta_land)))
    ]
    own = [(start, BLK) for start in range(0, slots, BLK)]
    order = [(kernel_ref, meta_ref, piece) for piece in own]
    order += [(taps_land, meta_land, (start, BLK)) for start in range(0, slots, BLK)]
    prepare(*order[0], buffers[0])
    for j in range(len(order)):
        if j == 1:
            pl.semaphore_wait(barrier, 1 + n_seat - 1 + n_bl - 1)
            for swap in swaps:
                swap.start()
        if j + 1 == len(own):
            for swap in swaps:
                swap.wait()
        if j + 1 < len(order):
            prepare(*order[j + 1], buffers[(j + 1) % 2])
        if j + 1 < len(order):
            scatter(buffers[j % 2], order[j][2][1], j == 0)
    last = (buffers[(len(order) - 1) % 2], order[-1][2][1], False)
    scatter(*last, (0, 1))

    msend_ref[...] = jnp.broadcast_to(jnp.sum(mom_ref[...], axis=1, keepdims=True), msend_ref.shape)
    def drain(ref, send, recv):
        pltpu.make_async_copy(ref, ref, send).wait()
        pltpu.make_async_copy(ref, ref, recv).wait()

    for d in range(1, n_seat):
        pltpu.make_async_remote_copy(
            src_ref=msend_ref, dst_ref=mxland_ref.at[d - 1], send_sem=xm_send, recv_sem=xm_recv,
            device_id=(seat_peer(d) * CORES + core, bl), device_id_type=MESH,
        ).start()

    for load in loads[9:]:
        load.wait()
    flipper = jnp.where(first, 1.0, -1.0)
    spin = [
        (jnp.where(first, 1.0, float(np.cos(two_pi * s / 8))), jnp.where(first, 0.0, float(np.sin(two_pi * s / 8))))
        for s in range(4)
    ]

    def transform(k):
        grid_ref = grid_refs[k]
        low_row = 0
        pieces = [[] for b in range(quads)]
        for p in range(planes):
            edges = []
            for b in range(quads):
                q = p * quads + b
                lanes = pl.ds(q % 2 * LANES, LANES)
                edges.append(grid_ref[q // 2, low_row + 64 : low_row + 72, lanes])
            edges = [pltpu.roll(edges[-1], 1, 1)] + edges[:-1]
            for b in range(quads):
                q = p * quads + b
                lanes = pl.ds(q % 2 * LANES, LANES)
                real = grid_ref[q // 2, low_row : low_row + 32, lanes]
                imag = grid_ref[q // 2, low_row + 32 : low_row + 64, lanes]
                edge = edges[b]
                head_real = real[:8] + jnp.where(first, edge, 0.0)
                head_imag = imag[:8] + jnp.where(first, pltpu.roll(edge, held, 0), 0.0)
                real = jnp.concatenate([head_real, real[8:]], axis=0)
                imag = jnp.concatenate([head_imag, imag[8:]], axis=0)
                pieces[b].append(jnp.concatenate([real, imag], axis=1))
        for b in range(quads):
            high, low = split(jnp.concatenate(pieces[b], axis=0))
            spec_ref[k, b] = (
                jnp.dot(high, coarse_ref[b, 0], preferred_element_type=jnp.float32)
                + jnp.dot(high, coarse_ref[b, 1], preferred_element_type=jnp.float32)
                + jnp.dot(low, coarse_ref[b, 0], preferred_element_type=jnp.float32)
            )

        def one_plane(p):
            inner = [[None] * pairs for r in range(4)]
            for t in range(pairs):
                column = []
                for b in range(quads):
                    row = pl.ds(p * 32 + t * 8, 8)
                    column.append((spec_ref[k, b, row, :LANES], spec_ref[k, b, row, LANES:]))
                for r, z in enumerate(radix4(column)):
                    inner[r][t] = multiply(z, (twist_ref[r, t, 0], twist_ref[r, t, 1]))
            for r in range(4):
                for s, z in enumerate(radix4(inner[r])):
                    if s:
                        z = multiply(z, spin[s])
                    real = pltpu.roll(z[0], held, 0) + z[0] * flipper
                    imag = pltpu.roll(z[1], held, 0) + z[1] * flipper
                    at = r + 4 * s
                    term = real * screen_ref[p, at, 0] - imag * screen_ref[p, at, 1]
                    acc_ref[k, at] = acc_ref[k, at] + term if p else term

        for p in range(planes):
            one_plane(p)
        for at in range(16):
            img_refs[k][pl.ds(at, 8, stride=16), :] = acc_ref[k, at]

    span = per * 16

    def send_x(k):
        for d in range(1, n_seat):
            for h in range(2):
                row = pl.multiple_of((held * h + seat_peer(d) * per) * 16, 16)
                pltpu.make_async_remote_copy(
                    src_ref=img_refs[k].at[pl.ds(row, span), :], dst_ref=xland_ref.at[k, d - 1, h],
                    send_sem=x_send.at[k], recv_sem=x_recv.at[k],
                    device_id=(seat_peer(d) * CORES + core, bl), device_id_type=MESH,
                ).start()

    def send_b(k):
        for d in range(1, n_bl):
            pltpu.make_async_remote_copy(
                src_ref=sum_ref.at[k, bl_peer(d)], dst_ref=bland_ref.at[k, d - 1],
                send_sem=b_send.at[k], recv_sem=b_recv.at[k],
                device_id=(chan, bl_peer(d)), device_id_type=MESH,
            ).start()

    share = per * NPIX // (n_bl * LANES)

    def gather_x(k):
        drain(xland_ref.at[k], x_send.at[k], x_recv.at[k])
        for h in range(2):
            row = pl.multiple_of((held * h + seat * per) * 16, 16)
            total = img_refs[k][pl.ds(row, span), :]
            for d in range(1, n_seat):
                total = total + xland_ref[k, d - 1, h]
            for i in range(per):
                at = (i * 32 + h * 16) // share
                sum_ref[k, at : at + 16 // share] = total[i * 16 : (i + 1) * 16].reshape(16 // share, share, LANES)
        send_b(k)

    for k in range(TAYLOR):
        if k == 0:
            scatter(*last, (2,))
        transform(k)
        send_x(k)
    drain(mxland_ref, xm_send, xm_recv)
    total = msend_ref[...]
    for d in range(1, n_seat):
        total = total + mxland_ref[d - 1]
    msum_ref[...] = total
    for d in range(1, n_bl):
        pltpu.make_async_remote_copy(
            src_ref=msum_ref, dst_ref=mland_ref.at[d - 1], send_sem=bm_send, recv_sem=bm_recv,
            device_id=(chan, bl_peer(d)), device_id_type=MESH,
        ).start()
    for k in range(TAYLOR):
        gather_x(k)

    drain(mland_ref, bm_send, bm_recv)
    moments = msum_ref[...]
    for d in range(1, n_bl):
        moments = moments + mland_ref[d - 1]
    images = []
    for k in range(TAYLOR):
        drain(bland_ref.at[k], b_send.at[k], b_recv.at[k])
        total = sum_ref[k, bl]
        for d in range(1, n_bl):
            total = total + bland_ref[k, d - 1]
        images.append(total)
    solved = solve_taylor([moments[m : m + 1] for m in range(MOMENTS)], images)
    for k in range(TAYLOR):
        out_ref[k] = solved[k]


def strip_image(n_chan, n_bl, count, offsets, value, weight, kernel, tiles, plane, chans):
    consts = [jnp.asarray(t) for t in tables(n_chan)]
    tap_table, coarse, twist, screen = consts
    vmem = pl.BlockSpec(memory_space=pltpu.VMEM)
    hbm = pl.BlockSpec(memory_space=pl.ANY)
    slots = kernel.shape[1]
    n_seat = n_chan // CORES
    per = STRIP // n_chan
    share = per * NPIX // (n_bl * LANES)
    f32 = jnp.float32
    bf16 = jnp.bfloat16
    dma = pltpu.SemaphoreType.DMA
    block = [((rows_all, BLK), bf16), ((rows_all, BLK), f8), ((BLK, planes * ntiles), f8)]
    inputs = (count, offsets, value, weight, kernel, tiles, plane, chans)
    scratch = [(x.shape, x.dtype) for x in inputs] + [
        (tap_table.shape[1:], bf16), (coarse.shape, bf16), (twist.shape, f32), (screen.shape[1:], f32),
        ((8, slots), f32), ((8, slots), f32), (kernel.shape, bf16),
        *block, *block,
        ((groups, per_k, 2 * LANES), f32), ((groups, per_k, 2 * LANES), f32), ((groups, per_k, 2 * LANES), f32), ((8, BLK), f32), ((TAYLOR, quads, planes * 32, 2 * LANES), f32),
        ((TAYLOR, 16, 8, LANES), f32), ((LANES, LANES), f32), ((LANES, LANES), f32), ((LANES, LANES), f32),
        ((TAYLOR, n_seat - 1, 2, per * 16, LANES), f32),
        ((TAYLOR, n_bl, share, LANES), f32), ((TAYLOR, n_bl - 1, share, LANES), f32),
        ((8, LANES), f32), ((n_seat - 1, 8, LANES), f32), ((8, LANES), f32), ((n_bl - 1, 8, LANES), f32),
    ]
    return pl.pallas_call(
        functools.partial(strip_kernel, n_chan, n_bl),
        out_shape=pltpu.VMEM((TAYLOR, share, LANES), f32),
        in_specs=[hbm] * (len(inputs) + len(consts)),
        out_specs=vmem,
        scratch_shapes=[pltpu.VMEM(shape, kind) for shape, kind in scratch]
        + [
            dma((len(inputs) + len(consts),)), dma((2,)), dma((2,)),
            dma((TAYLOR,)), dma((TAYLOR,)), dma, dma, dma((TAYLOR,)), dma((TAYLOR,)), dma, dma,
        ],
        compiler_params=pltpu.CompilerParams(
            vmem_limit_bytes=56 * 1024 * 1024, collective_id=0, has_side_effects=True
        ),
        name="strip_image",
    )(*inputs, *consts)


def solution(mesh):
    n_chan = mesh.shape["chan"]
    n_bl = mesh.shape["bl"]

    def body(vis_value, vis_weight, kernel, tile_index, plane_index, chan_index, chan_offset, counts):
        out = strip_image(
            n_chan, n_bl, counts, chan_offset, vis_value[0, 0], vis_weight[0], kernel[0, 0],
            tile_index[0], plane_index[0], chan_index[0],
        )
        return out.reshape(TAYLOR, -1)

    in_specs = (
        P("chan", "bl", None, None),
        P("chan", "bl", None),
        P("chan", "bl", None, None),
        P("chan", "bl", None),
        P("chan", "bl", None),
        P("chan", "bl", None),
        P("chan", None),
        P("chan", "bl"),
    )
    out_specs = P(None, ("chan", "bl"))
    return jax.shard_map(body, mesh=mesh, in_specs=in_specs, out_specs=out_specs, check_vma=False)
```
